32 devices in a mesh: tm: 16 (over z, x, core), tile: 2 (over y).
Axes of the slice: x: 2, y: 2, z: 4, core: 2. Of those that a mesh axis runs over, the one named last changes fastest.
Arguments:
- queries: bfloat16 [32, 4, 64, 2560], P('tm', 'tile'), may hold values from -40 to 40
- keys: bfloat16 [32, 4, 64, 2560], P('tm', 'tile'), may hold values from -6 to 6
- values: bfloat16 [32, 4, 64, 2560], P('tm', 'tile'), may hold values from -6 to 6
- neighbours: int32 [16, 2, 3], P('tm', 'tile'), may hold values from -1 to 14, as said below
- halo_rows: int32 [16, 2], P('tm', 'tile'), may hold values from 0 to 2, as said below
Outputs:
- attended: bfloat16 [32, 4, 64, 2560], P('tm', 'tile')
The draws below stay inside these ranges and needn't reach their ends.
Inputs may be any that keep to these rules, and one draw needn't show every extreme that they name: `neighbours`: for frame block b and tile t, the entries that are not -1 are distinct frame blocks from max(0, b - 5) to b - 1; lists hold 0 to 3 entries, and some list is full. `halo_rows`: some frame block and tile reads 2 rows.
All inputs are finite; a program needn't handle non-finite values.
Results may differ from the reference program's by a relative error of at most 0.0046.
Values may be sent and summed in bfloat16 or wider, within the bound.
A program may use at most 128 MiB of HBM per device.

```python
import math
import jax
import jax.numpy as jnp
from jax import lax

HEADS = 20
HD = 128
GRID_W = 64
FR_DEV = 2
TROWS = 2
HMAX = 2
NB = 3
WIN = 5
CHANNELS = 2560
BLOCKS = 16
TILES = 2
FRAMES = 32
GRID_H = 4


def drawn_pair(key):
    base = jax.random.fold_in(key, 11)
    query_seed, keys_seed = jax.random.split(base, 2)
    shape = (FRAMES, GRID_H, GRID_W, HEADS, HD)
    query_base = jnp.clip(jax.random.normal(query_seed, shape, jnp.float32), -6.0, 6.0)
    key_base = jnp.clip(jax.random.normal(keys_seed, shape, jnp.float32), -6.0, 6.0)
    flat_shape = (FRAMES, GRID_H, GRID_W, HEADS * HD)
    return (query_base.reshape(flat_shape), key_base.reshape(flat_shape))


def draw_queries(key, part):
    return drawn_pair(key)[0].astype(jnp.bfloat16)


def draw_keys(key, part):
    return drawn_pair(key)[1].astype(jnp.bfloat16)


def draw_neighbours(key, part):
    base = jax.random.fold_in(key, 31)
    bits_seed, length_seed = jax.random.split(base)
    random_bits = jax.random.randint(bits_seed, (BLOCKS, TILES, WIN), 0, 1 << 20)
    offsets = jnp.arange(1, WIN + 1, dtype=jnp.int32)
    block_pos = jnp.arange(BLOCKS, dtype=jnp.int32)[:, None, None]
    usable = block_pos - offsets[None, None, :] >= 0
    ranked = jnp.where(usable, random_bits * WIN + offsets - 1 + WIN, offsets - 1 + jnp.zeros_like(random_bits))
    top_vals, top_idx = lax.top_k(ranked, NB)
    chosen = top_idx.astype(jnp.int32) + 1
    list_length = jax.random.randint(length_seed, (BLOCKS, TILES), 0, NB + 1)
    list_length = list_length.at[BLOCKS - 1, 0].set(NB)
    slot_index = jnp.arange(NB, dtype=jnp.int32)[None, None, :]
    block_ids = block_pos - chosen
    kept_mask = (slot_index < list_length[:, :, None]) & (block_ids >= 0)
    return jnp.where(kept_mask, block_ids, -1).astype(jnp.int32)


def draw_halo_rows(key, part):
    widths = jax.random.randint(jax.random.fold_in(key, 23), (BLOCKS, TILES), 0, HMAX + 1)
    return widths.at[BLOCKS - 1, 0].set(HMAX).astype(jnp.int32)


def levels(key, shape, pieces, low, high):
    level, own = 1.0, jax.random.fold_in(key, 6)
    for axis_at, shards_of in pieces:
        draws = jnp.exp(jax.random.uniform(jax.random.fold_in(own, axis_at), (shards_of,), jnp.float32, low / len(pieces), high / len(pieces)))
        level = level * jnp.repeat(draws, shape[axis_at] // shards_of).reshape([-1 if axis == axis_at else 1 for axis in range(len(shape))])
    return level


def normal_values(key, shape, spread, bound, cuts=(), kind=jnp.bfloat16):
    factor_of = levels(key, shape, cuts, -0.22, 0.18) if cuts else 1.0
    array = jax.random.normal(key, shape, jnp.float32) * spread * factor_of
    return jnp.minimum(jnp.maximum(array, -bound), bound).astype(kind)


def setup_inputs(seed: int = 0) -> dict:
    key_list = jax.random.split(jax.random.key(seed), 6)
    return {
        "queries": draw_queries(jax.random.fold_in(key_list[5], 71), 0),
        "keys": draw_keys(jax.random.fold_in(key_list[5], 71), 0),
        "values": normal_values(key_list[2], (FRAMES, GRID_H, GRID_W, CHANNELS), 1.0, 6.0, ((0, 16), (1, 2))),
        "neighbours": draw_neighbours(jax.random.fold_in(key_list[5], 71), 0),
        "halo_rows": draw_halo_rows(jax.random.fold_in(key_list[5], 71), 0),
    }


def attend(query_rows, key_rows, value_rows, allowed):
    tokens, channels = query_rows.shape
    head_count = channels // HD
    key_count = key_rows.shape[0]
    query_heads = query_rows.astype(jnp.float32).reshape(tokens, head_count, HD)
    key_heads = key_rows.astype(jnp.float32).reshape(key_count, head_count, HD)
    value_heads = value_rows.astype(jnp.float32).reshape(key_count, head_count, HD)
    scores = jnp.einsum('qhd,khd->hqk', query_heads, key_heads) / math.sqrt(HD)
    scores = jnp.where(allowed[None], scores, -jnp.inf)
    maximum = lax.optimization_barrier(jnp.max(scores, axis=2, keepdims=True))
    weights = jnp.where(allowed[None], jnp.exp(scores - maximum), 0.0)
    totals = lax.optimization_barrier(jnp.sum(weights, axis=2))
    rounded = lax.optimization_barrier(weights.astype(jnp.bfloat16)).astype(jnp.float32)
    numerator = jnp.einsum('hqk,khd->qhd', rounded, value_heads)
    return (numerator / totals.T[:, :, None]).reshape(tokens, channels).astype(jnp.bfloat16)

def reference(queries, keys, values, neighbours, halo_rows):
    channels = queries.shape[3]
    tokens = FR_DEV * TROWS * GRID_W
    span_rows = TROWS + 2 * HMAX
    pad_keys = jnp.pad(keys, ((0, 0), (HMAX, HMAX), (0, 0), (0, 0)))
    pad_values = jnp.pad(values, ((0, 0), (HMAX, HMAX), (0, 0), (0, 0)))
    anchor = jnp.zeros((), jnp.int32)
    query_frame = lax.broadcasted_iota(jnp.int32, (FR_DEV, TROWS, GRID_W), 0).reshape(-1)
    key_frame = lax.broadcasted_iota(jnp.int32, (FR_DEV, span_rows, GRID_W), 0).reshape(-1)
    key_row = lax.broadcasted_iota(jnp.int32, (FR_DEV, span_rows, GRID_W), 1).reshape(-1)

    def one_device(device):
        block_index = (device // TILES).astype(jnp.int32)
        tile_index = (device % TILES).astype(jnp.int32)
        frame_start = (block_index * FR_DEV).astype(jnp.int32)
        row_start = (tile_index * TROWS).astype(jnp.int32)
        query_rows = lax.dynamic_slice(queries, (frame_start, row_start, anchor, anchor), (FR_DEV, TROWS, GRID_W, channels)).reshape(tokens, channels)
        own_keys = lax.dynamic_slice(pad_keys, (frame_start, row_start, anchor, anchor), (FR_DEV, span_rows, GRID_W, channels)).reshape(-1, channels)
        own_values = lax.dynamic_slice(pad_values, (frame_start, row_start, anchor, anchor), (FR_DEV, span_rows, GRID_W, channels)).reshape(-1, channels)
        listed = neighbours[block_index, tile_index]
        halo_reach = halo_rows[block_index, tile_index]

        def fetch_rows(block_id):
            start_frame = (jnp.maximum(block_id, 0) * FR_DEV).astype(jnp.int32)
            far_keys = lax.dynamic_slice(keys, (start_frame, row_start, anchor, anchor), (FR_DEV, TROWS, GRID_W, channels))
            far_values = lax.dynamic_slice(values, (start_frame, row_start, anchor, anchor), (FR_DEV, TROWS, GRID_W, channels))
            return (far_keys, far_values)
        far_keys, far_values = jax.vmap(fetch_rows)(listed)
        global_row = row_start - HMAX + key_row
        row_ok = (global_row >= 0) & (global_row < GRID_H) & (key_row >= HMAX - halo_reach) & (key_row < HMAX + TROWS + halo_reach)
        own_mask = (key_frame[None, :] <= query_frame[:, None]) & row_ok[None, :]
        slot_mask = jnp.repeat(listed >= 0, tokens)
        allowed = jnp.concatenate((own_mask, jnp.broadcast_to(slot_mask[None, :], (tokens, slot_mask.shape[0]))), axis=1)
        key_rows = jnp.concatenate((own_keys, far_keys.reshape(-1, channels)), axis=0)
        value_rows = jnp.concatenate((own_values, far_values.reshape(-1, channels)), axis=0)
        return attend(query_rows, key_rows, value_rows, allowed)
    results = lax.map(one_device, jnp.arange(BLOCKS * TILES, dtype=jnp.int32))
    results = results.reshape(BLOCKS, TILES, FR_DEV, TROWS, GRID_W, channels)
    return results.transpose(0, 2, 1, 3, 4, 5).reshape(FRAMES, GRID_H, GRID_W, channels)
```

```python
import functools
import math

import jax
import jax.numpy as jnp
from jax import lax
from jax.experimental import pallas as pl
from jax.experimental.pallas import tpu as pltpu
from jax.sharding import PartitionSpec as P

HD = 128
HMAX = 2
WIN = 5
GROUP = 4
ASKS = 2
FIRST = ASKS - 1
PAST = GROUP - FIRST
ROWS = 8
LOW = -1e30
SCALE = math.log2(math.e) / math.sqrt(HD)


def both(*terms):
    out = terms[0]
    for term in terms[1:]:
        out = jnp.logical_and(out, term)
    return out


def kernel(count, tiles, shape, lists_ref, halo_ref, q_ref, k_ref, v_ref, out_ref,
           own, side, past, ask, part, stat, back, back_stat, res, info, far, bias,
           local_sem, in_sem, in_send, side_sem, side_send, past_sem, past_send,
           ask_sem, ask_send, back_sem, back_send, stat_sem, stat_send,
           out_sem, out_send, info_sem, info_send, asked_sem, asked_send):
    frames, rows, columns = shape
    tokens = frames * rows * columns
    share = own.shape[1]
    slots = lists_ref.shape[0]
    block = lax.axis_index("tm")
    tile = lax.axis_index("tile")
    me = block % GROUP
    base = block - me
    partner = me + 1 - 2 * (me % 2)
    across = (me + 2) % GROUP
    beyond = (partner + 2) % GROUP
    behind = block >= GROUP
    ahead = block + GROUP < count

    def columns_of(head):
        return pl.ds(pl.multiple_of(head * HD, HD), HD)

    def remote(src, dst, send, recv, target):
        return pltpu.make_async_remote_copy(
            src_ref=src, dst_ref=dst, send_sem=send, recv_sem=recv,
            device_id=target, device_id_type=pl.DeviceIdType.MESH,
        )

    def landed(ref, sem):
        remote(ref, ref, in_send.at[0], sem, {"tm": block}).wait_recv()

    def sent(ref, sem):
        remote(ref, ref, sem, out_sem, {"tm": block}).wait_send()

    if tiles == 2:
        sides = [(tile >= 1, 1 - 2 * tile, None)]
    elif tiles > 2:
        sides = [(None, -1, tile >= 1), (None, 1, tile + 1 < tiles)]
    else:
        sides = []

    def maybe(condition, action):
        if condition is None:
            action()
        else:
            pl.when(condition)(action)

    def fetch(h, carry):
        for i, ref in enumerate((q_ref, k_ref, v_ref)):
            pltpu.make_async_copy(ref.at[:, columns_of(me * share + h)],
                                  own.at[me, h, i], local_sem.at[h]).start()
        return carry

    lax.fori_loop(0, share, fetch, 0)

    barrier = pltpu.get_barrier_semaphore()
    expected = jnp.int32(GROUP - 1)

    def greet(target):
        pl.semaphore_signal(barrier, inc=1, device_id=target, device_id_type=pl.DeviceIdType.MESH)

    for role in (partner, across, beyond):
        greet({"tm": base + role})
    for there, step in ((behind, -GROUP), (ahead, GROUP)):
        pl.when(there)(lambda: greet({"tm": block + step}))
        expected += there.astype(jnp.int32)
    for _, step, there in sides:
        maybe(there, lambda: greet({"tile": tile + step}))
        expected += 1 if there is None else there.astype(jnp.int32)

    row = lax.broadcasted_iota(jnp.int32, (ROWS, tokens), 0)
    mine = jnp.where(row == slots, halo_ref[0], -1)
    for n in range(slots):
        mine = jnp.where(row == n, lists_ref[n], mine)
    info[me] = mine

    pl.semaphore_wait(barrier, expected)

    for role in (partner, across, beyond):
        remote(info.at[me], info.at[me], info_send, info_sem.at[me], {"tm": base + role}).start()

    def give(role, at, h):
        for i, ref in ((1, k_ref), (2, v_ref), (0, q_ref)):
            remote(ref.at[:, columns_of(role * share + h)], own.at[me, h, i],
                   in_send.at[at], in_sem.at[me, h], {"tm": base + role}).start()

    def give_partner(h, carry):
        give(partner, 0, h)
        return carry

    def give_across(h):
        give(across, 1, h)
        give(beyond, 2, h)

    give_across(0)
    lax.fori_loop(0, share, give_partner, 0)
    give_across(1)

    def forward(role, h):
        pair = pl.ds(1, 2)
        for at, (_, step, there) in enumerate(sides):
            other = len(sides) - 1 - at
            maybe(there, lambda: remote(
                own.at[role, h, pair], side.at[other, role, h], side_send.at[at],
                side_sem.at[other, role, h], {"tile": tile + step}).start())

        @pl.when(both(role >= FIRST, ahead))
        def _():
            remote(own.at[role, h, pair], past.at[role - FIRST, h], past_send,
                   past_sem.at[role - FIRST, h], {"tm": block + GROUP}).start()

        @pl.when(both(role < ASKS, behind))
        def _():
            remote(own.at[role, h, 0], ask.at[role, h], ask_send,
                   ask_sem.at[role, h], {"tm": block - GROUP}).start()

    def forward_near(h):
        pltpu.make_async_copy(own.at[me, h], own.at[me, h], local_sem.at[h]).wait()
        forward(me, h)
        landed(own.at[partner, h], in_sem.at[partner, h])
        forward(partner, h)

    def forward_far(h):
        for role in (across, beyond):
            landed(own.at[role, h], in_sem.at[role, h])
            forward(role, h)

    forward_near(0)
    forward_near(1)

    @pl.when(jnp.logical_not(behind))
    def _():
        past[...] = jnp.zeros(past.shape, past.dtype)
        back[...] = jnp.zeros(back.shape, back.dtype)
        back_stat[...] = jnp.full(back_stat.shape, LOW, back_stat.dtype)

    for at, (_, _, there) in enumerate(sides):
        if there is not None:

            @pl.when(jnp.logical_not(there))
            def _():
                side[at] = jnp.zeros(side.shape[1:], side.dtype)

    for role in (partner, across, beyond):
        landed(info.at[role], info_sem.at[role])

    @pl.when(behind)
    def _():
        remote(info.at[pl.ds(0, ASKS)], info.at[pl.ds(GROUP, ASKS)], asked_send, asked_sem,
               {"tm": block - GROUP}).start()

    def spread(at, number):
        out = jnp.full((ROWS, tokens), LOW, jnp.float32)
        for d in range(1, WIN + 1):
            wanted = jnp.where(number >= d, number - d, -2)
            hit = info[at, 0:1, :] == wanted
            for n in range(1, slots):
                hit = jnp.logical_or(hit, info[at, n : n + 1, :] == wanted)
            out = jnp.where(jnp.logical_and(row == d, hit), 0.0, out)
        far[at] = out

    query = lax.broadcasted_iota(jnp.int32, (tokens, tokens), 0) // (rows * columns)
    key = lax.broadcasted_iota(jnp.int32, (tokens, tokens), 1)
    causal = key // (rows * columns) <= query
    bias[0] = jnp.where(causal, 0.0, LOW)
    key_row = (lax.broadcasted_iota(jnp.int32, (1, tokens), 1) // columns) % rows
    for role in range(GROUP):
        spread(role, base + role)
        reach = info[role, slots : slots + 1, :]
        above = jnp.where(key_row >= rows - reach, 0.0, LOW)
        below = jnp.where(key_row < reach, 0.0, LOW)
        for at, (upper, step, there) in enumerate(sides):
            if upper is not None:
                edge = jnp.where(upper, above, below)
            else:
                edge = jnp.where(there, above if step < 0 else below, LOW)
            bias[1 + role * len(sides) + at] = jnp.where(causal, edge, LOW)

    @pl.when(ahead)
    def _():
        landed(info.at[pl.ds(GROUP, ASKS)], asked_sem)
        for role in range(ASKS):
            spread(GROUP + role, base + GROUP + role)

    def attend(query_part, parts):
        scores = []
        most = None
        for k_part, _, shift in parts:
            s = lax.dot_general(query_part, k_part[...], (((1,), (1,)), ((), ())),
                                preferred_element_type=jnp.float32) + shift
            most = s if most is None else jnp.maximum(most, s)
            scores.append(s)
        top = jnp.max(most, axis=1, keepdims=True) * SCALE
        total = None
        numerator = None
        for s, (_, v_part, _) in zip(scores, parts):
            w = jnp.exp2(s * SCALE - top)
            total = w if total is None else total + w
            term = jnp.dot(w.astype(jnp.bfloat16), v_part[...], preferred_element_type=jnp.float32)
            numerator = term if numerator is None else numerator + term
        return numerator, jnp.sum(total, axis=1, keepdims=True), top

    def distant(at, d):
        return far[at, d : d + 1, :]

    def visit(h):
        for role in range(ASKS):
            landed(ask.at[role, h], ask_sem.at[role, h])
            parts = []
            for other in range(GROUP):
                d = role + GROUP - other
                if d <= WIN:
                    parts.append((own.at[other, h, 1], own.at[other, h, 2], distant(GROUP + role, d)))
            for other in range(GROUP - 1, GROUP):
                d = role + 2 * GROUP - other
                if d <= WIN:
                    kv = past.at[other - FIRST, h]
                    parts.append((kv.at[0], kv.at[1], distant(GROUP + role, d)))
            numerator, total, top = attend(ask[role, h], parts)
            part[role, h] = (numerator / total).astype(part.dtype)
            level = jnp.broadcast_to(top + jnp.log2(total), (tokens, HD))
            stat[role, h] = jnp.transpose(level)[0:1, :]
        for role in range(ASKS):
            remote(part.at[role, h], back.at[role, h], back_send, back_sem.at[role, h],
                   {"tm": block + GROUP}).start()
            remote(stat.at[role, h], back_stat.at[role, h], stat_send, stat_sem.at[role, h],
                   {"tm": block + GROUP}).start()

    def unit(role, h):
        for at, (_, _, there) in enumerate(sides):
            maybe(there, lambda: landed(side.at[at, role, h], side_sem.at[at, role, h]))
        if role < ASKS:

            @pl.when(behind)
            def _():
                landed(back.at[role, h], back_sem.at[role, h])
                landed(back_stat.at[role, h], stat_sem.at[role, h])

        parts = [(own.at[role, h, 1], own.at[role, h, 2], bias[0])]
        for other in range(role):
            parts.append((own.at[other, h, 1], own.at[other, h, 2], distant(role, role - other)))
        if role >= ASKS:
            for other in range(FIRST, GROUP):
                d = role + GROUP - other
                if d <= WIN:
                    kv = past.at[other - FIRST, h]
                    parts.append((kv.at[0], kv.at[1], distant(role, d)))
        for at in range(len(sides)):
            kv = side.at[at, role, h]
            parts.append((kv.at[0], kv.at[1], bias[1 + role * len(sides) + at]))
        numerator, total, top = attend(own[role, h, 0], parts)
        if role < ASKS:
            level = jnp.transpose(jnp.broadcast_to(back_stat[role, h], (HD, tokens)))
            peak = jnp.maximum(level, top)
            here = jnp.exp2(top - peak)
            there = jnp.exp2(level - peak)
            numerator = numerator * here + back[role, h].astype(jnp.float32) * there
            total = total * here + there
        res[role, h] = (numerator / total).astype(res.dtype)

    def deliver(role, h):
        place = columns_of(me * share + h)

        @pl.when(me == role)
        def _():
            out_ref[:, place] = res[role, h]

        @pl.when(me != role)
        def _():
            remote(res.at[role, h], out_ref.at[:, place], out_send, out_sem,
                   {"tm": base + role}).start()

    def answer(h):
        @pl.when(behind)
        def _():
            for at in range(PAST - 1):
                landed(past.at[at, h], past_sem.at[at, h])

        def half(phase, carry):
            pair = (me // 2 + 1 + phase) % 2
            for mine_ in range(2):

                @pl.when(pair == mine_)
                def _():
                    for role in (2 * mine_, 2 * mine_ + 1):
                        unit(role, h)
                    for role in (2 * mine_, 2 * mine_ + 1):
                        deliver(role, h)

            return carry

        lax.fori_loop(0, 2, half, 0)

    def step(t, carry):
        @pl.when(t + 2 < share)
        def _():
            give_across(t + 2)

        @pl.when(t < share)
        def _():
            forward_far(t)

        @pl.when(both(t % 2 == 0, 2 + t // 2 < share))
        def _():
            forward_near(2 + t // 2)

        @pl.when(both(t >= 1, t - 1 < share, behind))
        def _():
            landed(past.at[PAST - 1, t - 1], past_sem.at[PAST - 1, t - 1])

        @pl.when(both(t >= 1, t - 1 < share, ahead))
        def _():
            visit(t - 1)

        @pl.when(t >= 2)
        def _():
            answer(t - 2)

        return carry

    assert share >= 2 and 2 + (share + 1) // 2 >= share
    lax.fori_loop(0, share + 2, step, 0)

    landed(res.at[pl.ds(0, GROUP - 1)], out_sem)
    sent(res.at[pl.ds(0, GROUP - 1)], out_send)
    sent(info.at[pl.ds(0, GROUP - 1)], info_send)
    for at in range(GROUP - 1):
        sent(own.at[0], in_send.at[at])
    for at, (_, _, there) in enumerate(sides):
        maybe(there, lambda: sent(side.at[at], side_send.at[at]))

    @pl.when(ahead)
    def _():
        sent(past, past_send)
        sent(back, back_send)
        sent(back_stat, stat_send)

    @pl.when(behind)
    def _():
        sent(ask, ask_send)
        sent(info.at[pl.ds(0, ASKS)], asked_send)


def local(count, tiles, queries, keys, values, neighbours, halo_rows):
    frames, rows, columns, channels = queries.shape
    tokens = frames * rows * columns
    heads = channels // HD
    share = heads // GROUP
    assert rows == HMAX and count % GROUP == 0 and heads % GROUP == 0
    sides = min(2, tiles - 1)
    flat = (tokens, channels)
    piece = (tokens, HD)
    smem = pl.BlockSpec(memory_space=pltpu.SMEM)
    anywhere = pl.BlockSpec(memory_space=pl.ANY)
    dma = pltpu.SemaphoreType.DMA

    def vmem(*size, dtype=jnp.bfloat16):
        return pltpu.VMEM(size, dtype)

    out = pl.pallas_call(
        functools.partial(kernel, count, tiles, (frames, rows, columns)),
        out_shape=jax.ShapeDtypeStruct(flat, jnp.bfloat16),
        in_specs=[smem, smem, anywhere, anywhere, anywhere],
        out_specs=pl.BlockSpec(memory_space=pltpu.VMEM),
        scratch_shapes=[
            vmem(GROUP, share, 3, *piece),
            vmem(max(1, sides), GROUP, share, 2, *piece),
            vmem(PAST, share, 2, *piece),
            vmem(ASKS, share, *piece),
            vmem(ASKS, share, *piece),
            vmem(ASKS, share, 1, tokens, dtype=jnp.float32),
            vmem(ASKS, share, *piece),
            vmem(ASKS, share, 1, tokens, dtype=jnp.float32),
            vmem(GROUP, share, *piece),
            vmem(GROUP + ASKS, ROWS, tokens, dtype=jnp.int32),
            vmem(GROUP + ASKS, ROWS, tokens, dtype=jnp.float32),
            vmem(1 + GROUP * sides, tokens, tokens, dtype=jnp.float32),
            dma((share,)),
            dma((GROUP, share)),
            dma((GROUP - 1,)),
            dma((max(1, sides), GROUP, share)),
            dma((max(1, sides),)),
            dma((PAST, share)),
            dma,
            dma((ASKS, share)),
            dma,
            dma((ASKS, share)),
            dma,
            dma((ASKS, share)),
            dma,
            dma,
            dma,
            dma((GROUP,)),
            dma,
            dma,
            dma,
        ],
        compiler_params=pltpu.CompilerParams(
            collective_id=0, has_side_effects=True, vmem_limit_bytes=56 * 1024 * 1024
        ),
    )(
        neighbours.reshape(-1),
        halo_rows.reshape(-1),
        queries.reshape(flat),
        keys.reshape(flat),
        values.reshape(flat),
    )
    return out.reshape(queries.shape)


def solution(mesh):
    return jax.shard_map(
        functools.partial(local, mesh.shape["tm"], mesh.shape["tile"]),
        mesh=mesh,
        in_specs=(
            P("tm", "tile", None, None),
            P("tm", "tile", None, None),
            P("tm", "tile", None, None),
            P("tm", "tile", None),
            P("tm", "tile"),
        ),
        out_specs=P("tm", "tile", None, None),
        check_vma=False,
    )
```

```python
import functools
import math

import jax
import jax.numpy as jnp
from jax import lax
from jax.experimental import pallas as pl
from jax.experimental.pallas import tpu as pltpu
from jax.sharding import PartitionSpec as P

HD = 128
HMAX = 2
WIN = 5
GROUP = 4
ROWS = 8
LOW = -1e30
SCALE = math.log2(math.e) / math.sqrt(HD)


def both(*terms):
    out = terms[0]
    for term in terms[1:]:
        out = jnp.logical_and(out, term)
    return out


def kernel(count, tiles, shape, lists_ref, halo_ref, q_ref, k_ref, v_ref, out_ref,
           qs, kv, side, past, ask, part, stat, back, back_stat, res, info, far, bias,
           local_sem, q_sem, kv_sem, in_send, side_sem, side_send, past_sem, past_send,
           ask_sem, ask_send, back_sem, back_send, stat_sem, stat_send,
           out_sem, out_send, info_sem, info_send, asked_sem, asked_send):
    frames, rows, columns = shape
    tokens = frames * rows * columns
    share = kv.shape[1]
    slots = lists_ref.shape[0]
    block = lax.axis_index("tm")
    tile = lax.axis_index("tile")
    me = block % GROUP
    base = block - me
    partner = me + 1 - 2 * (me % 2)
    across = (me + 2) % GROUP
    beyond = (partner + 2) % GROUP
    behind = block >= GROUP
    ahead = block + GROUP < count
    last = GROUP - 1

    def columns_of(head):
        return pl.ds(pl.multiple_of(head * HD, HD), HD)

    def remote(src, dst, send, recv, target):
        return pltpu.make_async_remote_copy(
            src_ref=src, dst_ref=dst, send_sem=send, recv_sem=recv,
            device_id=target, device_id_type=pl.DeviceIdType.MESH,
        )

    def landed(ref, sem):
        remote(ref, ref, in_send.at[0], sem, {"tm": block}).wait_recv()

    def sent(ref, sem):
        remote(ref, ref, sem, out_sem, {"tm": block}).wait_send()

    if tiles == 2:
        sides = [(tile >= 1, 1 - 2 * tile, None)]
    elif tiles > 2:
        sides = [(None, -1, tile >= 1), (None, 1, tile + 1 < tiles)]
    else:
        sides = []

    def maybe(condition, action):
        if condition is None:
            action()
        else:
            pl.when(condition)(action)

    barrier = pltpu.get_barrier_semaphore()
    expected = jnp.int32(GROUP - 1)

    def greet(target):
        pl.semaphore_signal(barrier, inc=1, device_id=target, device_id_type=pl.DeviceIdType.MESH)

    for role in (across, beyond, partner):
        greet({"tm": base + role})
    for _, step, there in sides:
        maybe(there, lambda: greet({"tile": tile + step}))
        expected += 1 if there is None else there.astype(jnp.int32)
    for there, step in ((behind, -GROUP), (ahead, GROUP)):
        pl.when(there)(lambda: greet({"tm": block + step}))
        expected += there.astype(jnp.int32)

    def spots(role, h):
        return ((k_ref, kv.at[role, h, 0]), (v_ref, kv.at[role, h, 1]), (q_ref, qs.at[role, h]))

    def fetch(h, carry):
        for ref, spot in spots(me, h):
            pltpu.make_async_copy(ref.at[:, columns_of(me * share + h)], spot, local_sem.at[h]).start()
        return carry

    lax.fori_loop(0, share, fetch, 0)

    row = lax.broadcasted_iota(jnp.int32, (ROWS, tokens), 0)
    mine = jnp.where(row == slots, halo_ref[0], -1)
    for n in range(slots):
        mine = jnp.where(row == n, lists_ref[n], mine)
    info[me] = mine

    pl.semaphore_wait(barrier, expected)

    def give(role, at, h, which):
        for ref, spot in which(spots(me, h)):
            sem = q_sem if ref is q_ref else kv_sem
            remote(ref.at[:, columns_of(role * share + h)], spot, in_send.at[at], sem.at[me, h],
                   {"tm": base + role}).start()

    def keys_of(pairs):
        return pairs[:2]

    def queries_of(pairs):
        return pairs[2:]

    def give_across(h, which):
        give(across, 1, h, which)
        give(beyond, 2, h, which)

    def give_partner(h, carry):
        give(partner, 0, h, keys_of)
        give(partner, 0, h, queries_of)
        return carry

    def to_sides(role, h):
        for at, (_, step, there) in enumerate(sides):
            other = len(sides) - 1 - at
            maybe(there, lambda: remote(
                kv.at[role, h], side.at[other, role, h], side_send.at[at],
                side_sem.at[other, role, h], {"tile": tile + step}).start())

    def to_next(role, h):
        @pl.when(both(role == last, ahead))
        def _():
            remote(kv.at[role, h], past.at[h], past_send, past_sem.at[h],
                   {"tm": block + GROUP}).start()

    def to_before(role, h):
        @pl.when(behind)
        def _():
            remote(qs.at[role, h], ask.at[role, h], ask_send, ask_sem.at[role, h],
                   {"tm": block - GROUP}).start()

    def own_here(h):
        for _, spot in spots(me, h):
            pltpu.make_async_copy(spot, spot, local_sem.at[h]).wait()

    def partner_here(h):
        landed(kv.at[partner, h], kv_sem.at[partner, h])
        landed(qs.at[partner, h], q_sem.at[partner, h])

    def near_z(role, h):
        to_before(role, h)
        to_next(role, h)

    for role in (partner, across, beyond):
        remote(info.at[me], info.at[me], info_send, info_sem.at[me], {"tm": base + role}).start()
    give_across(0, keys_of)
    own_here(0)
    to_sides(me, 0)
    give_across(0, queries_of)
    give_across(1, queries_of)
    lax.fori_loop(0, share, give_partner, 0)
    if share > 2:
        give_across(2, queries_of)
    give_across(1, keys_of)
    near_z(me, 0)
    partner_here(0)
    to_sides(partner, 0)
    near_z(partner, 0)

    for role in (partner, across, beyond):
        landed(info.at[role], info_sem.at[role])

    @pl.when(behind)
    def _():
        remote(info.at[pl.ds(0, GROUP)], info.at[pl.ds(GROUP, GROUP)], asked_send, asked_sem,
               {"tm": block - GROUP}).start()

    def settle(h):
        own_here(h)
        near_z(me, h)
        partner_here(h)
        near_z(partner, h)

    def near_sides(h):
        to_sides(partner, h)
        to_sides(me, h)

    settle(1)
    near_sides(1)

    @pl.when(jnp.logical_not(behind))
    def _():
        past[...] = jnp.zeros(past.shape, past.dtype)
        back[...] = jnp.zeros(back.shape, back.dtype)
        back_stat[...] = jnp.full(back_stat.shape, LOW, back_stat.dtype)

    for at, (_, _, there) in enumerate(sides):
        if there is not None:

            @pl.when(jnp.logical_not(there))
            def _():
                side[at] = jnp.zeros(side.shape[1:], side.dtype)

    def spread(at, number):
        out = jnp.full((ROWS, tokens), LOW, jnp.float32)
        for d in range(1, WIN + 1):
            wanted = jnp.where(number >= d, number - d, -2)
            hit = info[at, 0:1, :] == wanted
            for n in range(1, slots):
                hit = jnp.logical_or(hit, info[at, n : n + 1, :] == wanted)
            out = jnp.where(jnp.logical_and(row == d, hit), 0.0, out)
        far[at] = out

    query = lax.broadcasted_iota(jnp.int32, (tokens, tokens), 0) // (rows * columns)
    key = lax.broadcasted_iota(jnp.int32, (tokens, tokens), 1)
    causal = key // (rows * columns) <= query
    bias[0] = jnp.where(causal, 0.0, LOW)
    key_row = (lax.broadcasted_iota(jnp.int32, (1, tokens), 1) // columns) % rows
    for role in range(GROUP):
        spread(role, base + role)
        reach = info[role, slots : slots + 1, :]
        above = jnp.where(key_row >= rows - reach, 0.0, LOW)
        below = jnp.where(key_row < reach, 0.0, LOW)
        for at, (upper, step, there) in enumerate(sides):
            if upper is not None:
                edge = jnp.where(upper, above, below)
            else:
                edge = jnp.where(there, above if step < 0 else below, LOW)
            bias[1 + role * len(sides) + at] = jnp.where(causal, edge, LOW)

    @pl.when(ahead)
    def _():
        landed(info.at[pl.ds(GROUP, GROUP)], asked_sem)
        for role in range(GROUP):
            spread(GROUP + role, base + GROUP + role)

    def attend(query_part, parts):
        scores = []
        most = None
        for pair, shift in parts:
            s = lax.dot_general(query_part, pair[0], (((1,), (1,)), ((), ())),
                                preferred_element_type=jnp.float32) + shift
            most = s if most is None else jnp.maximum(most, s)
            scores.append(s)
        top = jnp.max(most, axis=1, keepdims=True) * SCALE
        total = None
        numerator = None
        for s, (pair, _) in zip(scores, parts):
            w = jnp.exp2(s * SCALE - top)
            total = w if total is None else total + w
            term = jnp.dot(w.astype(jnp.bfloat16), pair[1], preferred_element_type=jnp.float32)
            numerator = term if numerator is None else numerator + term
        return numerator, jnp.sum(total, axis=1, keepdims=True), top

    def distant(at, d):
        return far[at, d : d + 1, :]

    def visit(roles, h):
        for role in roles:
            landed(ask.at[role, h], ask_sem.at[role, h])
            parts = []
            for other in range(GROUP):
                d = role + GROUP - other
                if d <= WIN:
                    parts.append((kv.at[other, h], distant(GROUP + role, d)))
            if role + 1 + GROUP <= WIN:
                pl.when(behind)(lambda: landed(past.at[h], past_sem.at[h]))
                parts.append((past.at[h], distant(GROUP + role, role + 1 + GROUP)))
            numerator, total, top = attend(ask[role, h], parts)
            part[role, h] = (numerator / total).astype(part.dtype)
            level = jnp.broadcast_to(top + jnp.log2(total), (tokens, HD))
            stat[role, h] = jnp.transpose(level)[0:1, :]
            remote(part.at[role, h], back.at[role, h], back_send, back_sem.at[role, h],
                   {"tm": block + GROUP}).start()
            remote(stat.at[role, h], back_stat.at[role, h], stat_send, stat_sem.at[role, h],
                   {"tm": block + GROUP}).start()

    def unit(role, h):
        parts = [(kv.at[role, h], bias[0])]
        for other in range(role):
            parts.append((kv.at[other, h], distant(role, role - other)))

        @pl.when(behind)
        def _():
            landed(back.at[role, h], back_sem.at[role, h])
            landed(back_stat.at[role, h], stat_sem.at[role, h])

        for at, (_, _, there) in enumerate(sides):
            maybe(there, lambda: landed(side.at[at, role, h], side_sem.at[at, role, h]))
        for at in range(len(sides)):
            parts.append((side.at[at, role, h], bias[1 + role * len(sides) + at]))
        found = [attend(qs[role, h], parts)]
        level = jnp.transpose(jnp.broadcast_to(back_stat[role, h], (HD, tokens)))
        peak = level
        for _, _, top in found:
            peak = jnp.maximum(peak, top)
        total = jnp.exp2(level - peak)
        numerator = back[role, h].astype(jnp.float32) * total
        for number, amount, top in found:
            scale = jnp.exp2(top - peak)
            numerator += number * scale
            total += amount * scale
        res[role, h] = (numerator / total).astype(res.dtype)
        place = columns_of(me * share + h)

        @pl.when(me == role)
        def _():
            out_ref[:, place] = res[role, h]

        @pl.when(me != role)
        def _():
            remote(res.at[role, h], out_ref.at[:, place], out_send, out_sem,
                   {"tm": base + role}).start()

    def rest(t):
        def one(n, carry):
            turn = jnp.where(n == 0, across, jnp.where(n == 1, beyond, jnp.where(n == 3, partner, me)))
            for role in range(GROUP):
                pl.when(both(n != 2, t >= 1, turn == role))(lambda: unit(role, t - 1))

            pl.when(both(n == 2, t < share, ahead))(lambda: visit((0,), t))
            return carry

        lax.fori_loop(0, GROUP + 1, one, 0)

    def query_here(h):
        for role in (across, beyond):
            landed(qs.at[role, h], q_sem.at[role, h])
            to_before(role, h)

    def step(t, carry):
        @pl.when(t + 3 < share)
        def _():
            give_across(t + 3, queries_of)

        @pl.when(t + 2 < share)
        def _():
            give_across(t + 2, keys_of)
            settle(t + 2)

        @pl.when(t < share)
        def _():
            for role in (across, beyond):
                landed(kv.at[role, t], kv_sem.at[role, t])
                to_sides(role, t)
                to_next(role, t)

        @pl.when(both(t % 2 == 0, 2 + t // 2 < share))
        def _():
            near_sides(2 + t // 2)

        @pl.when(t < share)
        def _():
            pl.when(t == 0)(lambda: query_here(t))
            pl.when(t + 1 < share)(lambda: query_here(t + 1))
            pl.when(ahead)(lambda: visit(range(1, GROUP), t))
            pl.when(both(behind, jnp.logical_not(ahead)))(lambda: landed(past.at[t], past_sem.at[t]))

        rest(t)

        return carry

    assert share >= 2 and 2 + (share + 1) // 2 >= share
    lax.fori_loop(0, share + 1, step, 0)

    landed(res.at[pl.ds(0, GROUP - 1)], out_sem)
    sent(res.at[pl.ds(0, GROUP - 1)], out_send)
    sent(info.at[pl.ds(0, GROUP - 1)], info_send)
    for at in range(GROUP - 1):
        sent(qs.at[0], in_send.at[at])
        sent(kv.at[0], in_send.at[at])
    for at, (_, _, there) in enumerate(sides):
        maybe(there, lambda: sent(side.at[at], side_send.at[at]))

    @pl.when(ahead)
    def _():
        sent(back, back_send)
        sent(past, past_send)
        sent(back_stat, stat_send)

    @pl.when(behind)
    def _():
        sent(ask, ask_send)
        sent(info.at[pl.ds(0, GROUP)], asked_send)


def local(count, tiles, queries, keys, values, neighbours, halo_rows):
    frames, rows, columns, channels = queries.shape
    tokens = frames * rows * columns
    heads = channels // HD
    share = heads // GROUP
    assert rows == HMAX and count % GROUP == 0 and heads % GROUP == 0
    sides = min(2, tiles - 1)
    flat = (tokens, channels)
    piece = (tokens, HD)
    smem = pl.BlockSpec(memory_space=pltpu.SMEM)
    anywhere = pl.BlockSpec(memory_space=pltpu.HBM)
    dma = pltpu.SemaphoreType.DMA

    def vmem(*size, dtype=jnp.bfloat16):
        return pltpu.VMEM(size, dtype)

    out = pl.pallas_call(
        functools.partial(kernel, count, tiles, (frames, rows, columns)),
        out_shape=pltpu.VMEM(flat, jnp.bfloat16),
        in_specs=[smem, smem, anywhere, anywhere, anywhere],
        out_specs=pl.BlockSpec(memory_space=pltpu.VMEM),
        scratch_shapes=[
            vmem(GROUP, share, *piece),
            vmem(GROUP, share, 2, *piece),
            vmem(max(1, sides), GROUP, share, 2, *piece),
            vmem(share, 2, *piece),
            vmem(GROUP, share, *piece),
            vmem(GROUP, share, *piece),
            vmem(GROUP, share, 1, tokens, dtype=jnp.float32),
            vmem(GROUP, share, *piece),
            vmem(GROUP, share, 1, tokens, dtype=jnp.float32),
            vmem(GROUP, share, *piece),
            vmem(2 * GROUP, ROWS, tokens, dtype=jnp.int32),
            vmem(2 * GROUP, ROWS, tokens, dtype=jnp.float32),
            vmem(1 + GROUP * sides, tokens, tokens, dtype=jnp.float32),
            dma((share,)),
            dma((GROUP, share)),
            dma((GROUP, share)),
            dma((GROUP - 1,)),
            dma((max(1, sides), GROUP, share)),
            dma((max(1, sides),)),
            dma((share,)),
            dma,
            dma((GROUP, share)),
            dma,
            dma((GROUP, share)),
            dma,
            dma((GROUP, share)),
            dma,
            dma,
            dma,
            dma((GROUP,)),
            dma,
            dma,
            dma,
        ],
        compiler_params=pltpu.CompilerParams(
            collective_id=0, has_side_effects=True, vmem_limit_bytes=56 * 1024 * 1024
        ),
    )(
        neighbours.reshape(-1),
        halo_rows.reshape(-1),
        queries.reshape(flat),
        keys.reshape(flat),
        values.reshape(flat),
    )
    return out.reshape(queries.shape)


def solution(mesh):
    return jax.shard_map(
        functools.partial(local, mesh.shape["tm"], mesh.shape["tile"]),
        mesh=mesh,
        in_specs=(
            P("tm", "tile", None, None),
            P("tm", "tile", None, None),
            P("tm", "tile", None, None),
            P("tm", "tile", None),
            P("tm", "tile"),
        ),
        out_specs=P("tm", "tile", None, None),
        check_vma=False,
    )
```

```python
import functools
import math

import jax
import jax.numpy as jnp
from jax import lax
from jax.experimental import pallas as pl
from jax.experimental.pallas import tpu as pltpu
from jax.sharding import PartitionSpec as P

HD = 128
HMAX = 2
WIN = 5
GROUP = 4
FAR, NEAR, MINE = range(3)
Q_SENT, KV_SENT, RES_SENT, INFO_SENT, ASK_SENT, ASKED_SENT, PAST_SENT, BACK_SENT = range(8)
STAT_SENT = BACK_SENT + 2
KINDS = STAT_SENT + 2
ROWS = 8
LOW = -1e30
SCALE = math.log2(math.e) / math.sqrt(HD)


def both(*terms):
    out = terms[0]
    for term in terms[1:]:
        out = jnp.logical_and(out, term)
    return out


def kernel(count, tiles, shape, lists_ref, halo_ref, q_ref, k_ref, v_ref, out_ref,
           qs, kv, side, past, ask, part, stat, back, back_stat, res, info, far, bias,
           send, side_send, local_sem, near_sem, q_sem, kv_sem, side_sem, past_sem, ask_sem,
           back_sem, stat_sem, out_sem, info_sem):
    frames, rows, columns = shape
    tokens = frames * rows * columns
    share = kv.shape[1]
    slots = lists_ref.shape[0]
    block = lax.axis_index("tm")
    tile = lax.axis_index("tile")
    me = block % GROUP
    base = block - me
    partner = me + 1 - 2 * (me % 2)
    across = (me + 2) % GROUP
    beyond = (partner + 2) % GROUP
    behind = block >= GROUP
    ahead = block + GROUP < count
    last = GROUP - 1
    first_chip = me < 2
    early = (me == last).astype(jnp.int32)

    def columns_of(head):
        return pl.ds(pl.multiple_of(head * HD, HD), HD)

    def remote(src, dst, sender, recv, target):
        return pltpu.make_async_remote_copy(
            src_ref=src, dst_ref=dst, send_sem=sender, recv_sem=recv,
            device_id=target, device_id_type=pl.DeviceIdType.MESH,
        )

    def landed(ref, sem):
        remote(ref, ref, send.at[0], sem, {"tm": block}).wait_recv()

    def sent(ref, sem):
        remote(ref, ref, sem, out_sem, {"tm": block}).wait_send()

    if tiles == 2:
        sides = [(tile >= 1, 1 - 2 * tile, None)]
    elif tiles > 2:
        sides = [(None, -1, tile >= 1), (None, 1, tile + 1 < tiles)]
    else:
        sides = []

    def maybe(condition, action):
        if condition is None:
            action()
        else:
            pl.when(condition)(action)

    barrier = pltpu.get_barrier_semaphore()
    expected = jnp.int32(GROUP - 1)

    def greet(target):
        pl.semaphore_signal(barrier, inc=1, device_id=target, device_id_type=pl.DeviceIdType.MESH)

    for role in (across, beyond, partner):
        greet({"tm": base + role})
    for _, step, there in sides:
        maybe(there, lambda: greet({"tile": tile + step}))
        expected += 1 if there is None else there.astype(jnp.int32)
    for there, step in ((behind, -GROUP), (ahead, GROUP)):
        pl.when(there)(lambda: greet({"tm": block + step}))
        expected += there.astype(jnp.int32)

    def spots(h):
        return ((k_ref, kv.at[me, h, 0]), (v_ref, kv.at[me, h, 1]), (q_ref, qs.at[me, h]))

    def fetch(h, carry):
        for ref, spot in spots(h):
            pltpu.make_async_copy(ref.at[:, columns_of(me * share + h)], spot, local_sem).start()
        return carry

    lax.fori_loop(0, share, fetch, 0)

    row = lax.broadcasted_iota(jnp.int32, (ROWS, tokens), 0)
    mine = jnp.where(row == slots, halo_ref[0], -1)
    for n in range(slots):
        mine = jnp.where(row == n, lists_ref[n], mine)
    info[me] = mine

    pl.semaphore_wait(barrier, expected)

    def give(role, h, pairs, sem):
        for ref, spot in pairs:
            kind = Q_SENT if ref is q_ref else KV_SENT
            remote(ref.at[:, columns_of(role * share + h)], spot, send.at[kind], sem,
                   {"tm": base + role}).start()

    def give_keys(h):
        for role in (across, beyond):
            give(role, h, spots(h)[:2], kv_sem.at[early, h])

    def give_queries(h):
        for role in (across, beyond):
            give(role, h, spots(h)[2:], q_sem.at[early, h])

    def to_sides(role, kind, h):
        for at, (_, step, there) in enumerate(sides):
            other = len(sides) - 1 - at
            maybe(there, lambda: remote(
                kv.at[role, h], side.at[other, role, h], side_send.at[at],
                side_sem.at[other, kind, h], {"tile": tile + step}).start())

    def to_next(role, h):
        @pl.when(both(role == last, ahead))
        def _():
            remote(kv.at[role, h], past.at[h], send.at[PAST_SENT], past_sem.at[h],
                   {"tm": block + GROUP}).start()

    def to_before(role, h):
        sem = ask_sem.at[role // last, h]

        @pl.when(behind)
        def _():
            remote(qs.at[role, h], ask.at[role, h], send.at[ASK_SENT], sem,
                   {"tm": block - GROUP}).start()

    def near_z(h):
        for role in (me, partner):
            to_before(role, h)
            to_next(role, h)

    for role in (across, beyond, partner):
        remote(info.at[me], info.at[me], send.at[INFO_SENT], info_sem.at[0],
               {"tm": base + role}).start()
    give_keys(0)
    pltpu.make_async_copy(kv.at[me], kv.at[me], local_sem).wait()
    pltpu.make_async_copy(qs.at[me], qs.at[me], local_sem).wait()
    to_sides(me, MINE, 0)
    for h in range(2):
        give_queries(h)
    give(partner, 0, spots(0), near_sem.at[0])

    def give_rest(h, carry):
        give(partner, h, spots(h), near_sem.at[1])
        return carry

    def give_far(h, carry):
        pl.when(both(me != last, h + 1 < share))(lambda: give_queries(h + 1))
        give_keys(h)
        pl.when(both(me == last, h >= 2))(lambda: give_queries(h))
        return carry

    lax.fori_loop(1, share, give_rest, 0)
    lax.fori_loop(1, share, give_far, 0)
    landed(res.at[pl.ds(0, 3), 0], near_sem.at[0])
    to_sides(partner, NEAR, 0)
    near_z(0)

    landed(info.at[pl.ds(0, GROUP - 1)], info_sem.at[0])

    @pl.when(behind)
    def _():
        remote(info.at[pl.ds(0, GROUP)], info.at[pl.ds(GROUP, GROUP)], send.at[ASKED_SENT],
               info_sem.at[1], {"tm": block - GROUP}).start()

    landed(res.at[pl.ds(0, 3), pl.ds(0, share - 1)], near_sem.at[1])

    def near_sides(h):
        to_sides(partner, NEAR, h)
        to_sides(me, MINE, h)

    near_sides(1)

    @pl.when(jnp.logical_not(behind))
    def _():
        past[...] = jnp.zeros(past.shape, past.dtype)
        back[...] = jnp.zeros(back.shape, back.dtype)
        back_stat[...] = jnp.full(back_stat.shape, LOW, back_stat.dtype)

    for at, (_, _, there) in enumerate(sides):
        if there is not None:

            @pl.when(jnp.logical_not(there))
            def _():
                side[at] = jnp.zeros(side.shape[1:], side.dtype)

    def spread(at, number):
        out = jnp.full((ROWS, tokens), LOW, jnp.float32)
        for d in range(1, WIN + 1):
            wanted = jnp.where(number >= d, number - d, -2)
            hit = info[at, 0:1, :] == wanted
            for n in range(1, slots):
                hit = jnp.logical_or(hit, info[at, n : n + 1, :] == wanted)
            out = jnp.where(jnp.logical_and(row == d, hit), 0.0, out)
        far[at] = out

    query = lax.broadcasted_iota(jnp.int32, (tokens, tokens), 0) // (rows * columns)
    key = lax.broadcasted_iota(jnp.int32, (tokens, tokens), 1)
    causal = key // (rows * columns) <= query
    bias[0] = jnp.where(causal, 0.0, LOW)
    key_row = (lax.broadcasted_iota(jnp.int32, (1, tokens), 1) // columns) % rows
    for role in range(GROUP):
        spread(role, base + role)
        reach = info[role, slots : slots + 1, :]
        above = jnp.where(key_row >= rows - reach, 0.0, LOW)
        below = jnp.where(key_row < reach, 0.0, LOW)
        for at, (upper, step, there) in enumerate(sides):
            if upper is not None:
                edge = jnp.where(upper, above, below)
            else:
                edge = jnp.where(there, above if step < 0 else below, LOW)
            bias[1 + role * len(sides) + at] = jnp.where(causal, edge, LOW)

    @pl.when(ahead)
    def _():
        landed(info.at[pl.ds(GROUP, GROUP)], info_sem.at[1])

        for role in range(GROUP):
            spread(GROUP + role, base + GROUP + role)

    def attend(query_part, parts):
        scores = []
        most = None
        for pair, shift in parts:
            s = lax.dot_general(query_part, pair[0], (((1,), (1,)), ((), ())),
                                preferred_element_type=jnp.float32) + shift
            most = s if most is None else jnp.maximum(most, s)
            scores.append(s)
        top = jnp.max(most, axis=1, keepdims=True) * SCALE
        total = None
        numerator = None
        for s, (pair, _) in zip(scores, parts):
            w = jnp.exp2(s * SCALE - top)
            total = w if total is None else total + w
            term = jnp.dot(w.astype(jnp.bfloat16), pair[1], preferred_element_type=jnp.float32)
            numerator = term if numerator is None else numerator + term
        return numerator, jnp.sum(total, axis=1, keepdims=True), top

    def distant(at, d):
        return far[at, d : d + 1, :]

    def visit(role, h):
        parts = []
        for other in range(GROUP):
            d = role + GROUP - other
            if d <= WIN:
                parts.append((kv.at[other, h], distant(GROUP + role, d)))
        if role + 1 + GROUP <= WIN:
            pl.when(behind)(lambda: landed(past.at[h], past_sem.at[h]))
            parts.append((past.at[h], distant(GROUP + role, role + 1 + GROUP)))
        numerator, total, top = attend(ask[role, h], parts)
        part[role, h] = (numerator / total).astype(part.dtype)
        level = jnp.broadcast_to(top + jnp.log2(total), (tokens, HD))
        stat[role, h] = jnp.transpose(level)[0:1, :]
        kind = role // 2
        remote(part.at[role, h], back.at[role, h], send.at[BACK_SENT + kind], back_sem.at[kind, h],
               {"tm": block + GROUP}).start()
        remote(stat.at[role, h], back_stat.at[role, h], send.at[STAT_SENT + kind],
               stat_sem.at[kind, h], {"tm": block + GROUP}).start()

    two = pl.ds(0, 2)

    def returned(kind, h):
        landed(back.at[two, h], back_sem.at[kind, h])
        landed(back_stat.at[two, h], stat_sem.at[kind, h])

    def sides_here(kind, h):
        roles = {FAR: two, NEAR: partner, MINE: me}[kind]
        for at, (_, _, there) in enumerate(sides):
            maybe(there, lambda: landed(side.at[at, roles, h], side_sem.at[at, kind, h]))

    def unit(role, h, between=None):
        parts = [(kv.at[role, h], bias[0])]
        for other in range(role):
            parts.append((kv.at[other, h], distant(role, role - other)))
        margins = [(side.at[at, role, h], bias[1 + role * len(sides) + at]) for at in range(len(sides))]
        found = []
        if between is not None:
            found.append(attend(qs[role, h], parts))
            parts = []
            between()
        parts += margins
        if parts:
            found.append(attend(qs[role, h], parts))
        level = jnp.transpose(jnp.broadcast_to(back_stat[role, h], (HD, tokens)))
        peak = level
        for _, _, top in found:
            peak = jnp.maximum(peak, top)
        total = jnp.exp2(level - peak)
        numerator = back[role, h].astype(jnp.float32) * total
        for number, amount, top in found:
            scale = jnp.exp2(top - peak)
            numerator += number * scale
            total += amount * scale
        res[role, h] = (numerator / total).astype(res.dtype)
        place = columns_of(me * share + h)

        @pl.when(me == role)
        def _():
            out_ref[:, place] = res[role, h]

        @pl.when(me != role)
        def _():
            remote(res.at[role, h], out_ref.at[:, place], send.at[RES_SENT], out_sem,
                   {"tm": base + role}).start()

    def rest(t):
        h = t - 1

        def one(n, carry):
            turn = jnp.where(n == 0, across, jnp.where(n == 1, beyond, jnp.where(n == 3, partner, me)))
            final = both(n == GROUP, t == share)

            @pl.when(t >= 1)
            def _():
                pl.when(both(n == 0, behind))(lambda: returned(1 - me // 2, h))
                pl.when(both(n == 3, behind))(lambda: returned(me // 2, h))
                pl.when(n == 0)(lambda: sides_here(FAR, h))
                pl.when(n == 3)(lambda: sides_here(NEAR, h))
                pl.when(both(n == GROUP, t < share))(lambda: sides_here(MINE, h))

            for role in range(GROUP):
                pl.when(both(n != 2, t >= 1, turn == role, jnp.logical_not(final)))(
                    lambda: unit(role, h))
                pl.when(both(final, turn == role))(
                    lambda: unit(role, h, lambda: sides_here(MINE, h)))

            pl.when(both(n == 2, t + 1 < share, first_chip))(lambda: early_keys(t + 1))

            @pl.when(both(n == 2, t < share, ahead))
            def _():
                landed(ask.at[last, t], ask_sem.at[1, t])
                visit(last, t)
                visit(0, t)

            return carry

        lax.fori_loop(0, GROUP + 1, one, 0)

    def early_keys(h):
        landed(kv.at[last, h], kv_sem.at[1, h])
        to_next(last, h)
        to_sides(last, FAR, h)

    def late_queries(h):
        landed(qs.at[last, h], q_sem.at[1, h])
        to_before(last, h)

    def keys_here(h):
        @pl.when(first_chip)
        def _():
            landed(kv.at[2, h], kv_sem.at[0, h])
            to_sides(2, FAR, h)

        @pl.when(jnp.logical_not(first_chip))
        def _():
            landed(kv.at[two, h], kv_sem.at[0, h])
            for role in range(2):
                to_sides(role, FAR, h)

    def query_here(h):
        @pl.when(first_chip)
        def _():
            landed(qs.at[2, h], q_sem.at[0, h])
            to_before(2, h)

        @pl.when(jnp.logical_not(first_chip))
        def _():
            landed(qs.at[two, h], q_sem.at[0, h])
            for role in range(2):
                to_before(role, h)

    def step(t, carry):
        @pl.when(t < share)
        def _():
            @pl.when(both(t == 0, first_chip))
            def _():
                early_keys(t)

            keys_here(t)
            pl.when(t + 3 < share)(lambda: near_sides(t + 2))
            pl.when(both(t + 1 == share, share > 2))(lambda: near_sides(t))

            @pl.when(t == 0)
            def _():
                query_here(t)
                pl.when(first_chip)(lambda: late_queries(t))

            @pl.when(t + 1 < share)
            def _():
                query_here(t + 1)
                near_z(t + 1)

            @pl.when(ahead)
            def _():
                landed(ask.at[pl.ds(0, last), t], ask_sem.at[0, t])
                for role in range(1, last):
                    visit(role, t)

            pl.when(both(behind, jnp.logical_not(ahead)))(lambda: landed(past.at[t], past_sem.at[t]))

        rest(t)
        pl.when(both(t + 1 < share, first_chip))(lambda: late_queries(t + 1))
        return carry

    lax.fori_loop(0, share + 1, step, 0)

    peers = pl.ds(0, GROUP - 1)
    landed(res.at[peers], out_sem)
    sent(res.at[peers], send.at[RES_SENT])
    sent(info.at[peers], send.at[INFO_SENT])
    sent(qs.at[peers], send.at[Q_SENT])
    sent(kv.at[peers], send.at[KV_SENT])
    for at, (_, _, there) in enumerate(sides):
        maybe(there, lambda: sent(side.at[at], side_send.at[at]))

    @pl.when(ahead)
    def _():
        sent(past, send.at[PAST_SENT])
        for kind in range(2):
            sent(back.at[two], send.at[BACK_SENT + kind])
            sent(back_stat.at[two], send.at[STAT_SENT + kind])

    @pl.when(behind)
    def _():
        sent(ask, send.at[ASK_SENT])
        sent(info.at[pl.ds(0, GROUP)], send.at[ASKED_SENT])


def local(count, tiles, queries, keys, values, neighbours, halo_rows):
    frames, rows, columns, channels = queries.shape
    tokens = frames * rows * columns
    heads = channels // HD
    share = heads // GROUP
    assert rows == HMAX and count % GROUP == 0 and heads % GROUP == 0
    sides = min(2, tiles - 1)
    flat = (tokens, channels)
    piece = (tokens, HD)
    smem = pl.BlockSpec(memory_space=pltpu.SMEM)
    anywhere = pl.BlockSpec(memory_space=pltpu.HBM)
    dma = pltpu.SemaphoreType.DMA

    def vmem(*size, dtype=jnp.bfloat16):
        return pltpu.VMEM(size, dtype)

    out = pl.pallas_call(
        functools.partial(kernel, count, tiles, (frames, rows, columns)),
        out_shape=pltpu.VMEM(flat, jnp.bfloat16),
        in_specs=[smem, smem, anywhere, anywhere, anywhere],
        out_specs=pl.BlockSpec(memory_space=pltpu.VMEM),
        scratch_shapes=[
            vmem(GROUP, share, *piece),
            vmem(GROUP, share, 2, *piece),
            vmem(max(1, sides), GROUP, share, 2, *piece),
            vmem(share, 2, *piece),
            vmem(GROUP, share, *piece),
            vmem(GROUP, share, *piece),
            vmem(GROUP, share, 1, tokens, dtype=jnp.float32),
            vmem(GROUP, share, *piece),
            vmem(GROUP, share, 1, tokens, dtype=jnp.float32),
            vmem(GROUP, share, *piece),
            vmem(2 * GROUP, ROWS, tokens, dtype=jnp.int32),
            vmem(2 * GROUP, ROWS, tokens, dtype=jnp.float32),
            vmem(1 + GROUP * sides, tokens, tokens, dtype=jnp.float32),
            dma((KINDS,)),
            dma((max(1, sides),)),
            dma,
            dma((2,)),
            dma((2, share)),
            dma((2, share)),
            dma((max(1, sides), 3, share)),
            dma((share,)),
            dma((2, share)),
            dma((2, share)),
            dma((2, share)),
            dma,
            dma((2,)),
        ],
        compiler_params=pltpu.CompilerParams(
            collective_id=0, has_side_effects=True, vmem_limit_bytes=56 * 1024 * 1024
        ),
    )(
        neighbours.reshape(-1),
        halo_rows.reshape(-1),
        queries.reshape(flat),
        keys.reshape(flat),
        values.reshape(flat),
    )
    return out.reshape(queries.shape)


def solution(mesh):
    return jax.shard_map(
        functools.partial(local, mesh.shape["tm"], mesh.shape["tile"]),
        mesh=mesh,
        in_specs=(
            P("tm", "tile", None, None),
            P("tm", "tile", None, None),
            P("tm", "tile", None, None),
            P("tm", "tile", None),
            P("tm", "tile"),
        ),
        out_specs=P("tm", "tile", None, None),
        check_vma=False,
    )
```

```python
import functools
import math

import jax
import jax.numpy as jnp
from jax import lax
from jax.experimental import pallas as pl
from jax.experimental.pallas import tpu as pltpu
from jax.sharding import PartitionSpec as P

HD = 128
HMAX = 2
WIN = 5
GROUP = 4
FAR, NEAR, MINE = range(3)
Q_SENT, KV_SENT, RES_SENT, INFO_SENT, ASK_SENT, ASKED_SENT, PAST_SENT, BACK_SENT = range(8)
STAT_SENT = BACK_SENT + 2
KINDS = STAT_SENT + 2
ROWS = 8
LOW = -1e30
SCALE = math.log2(math.e) / math.sqrt(HD)


def both(*terms):
    out = terms[0]
    for term in terms[1:]:
        out = jnp.logical_and(out, term)
    return out


def kernel(count, tiles, shape, lists_hbm, halo_hbm, q_ref, k_ref, v_ref, out_ref,
           lists_ref, halo_ref,
           qs, kv, side, past, ask, part, stat, back, back_stat, res, info, far, bias,
           small_sem, send, side_send, local_sem, near_sem, q_sem, kv_sem, side_sem, past_sem, ask_sem,
           back_sem, stat_sem, out_sem, info_sem):
    frames, rows, columns = shape
    tokens = frames * rows * columns
    share = kv.shape[1]
    slots = lists_ref.shape[2]
    block = lax.axis_index("tm")
    tile = lax.axis_index("tile")
    me = block % GROUP
    base = block - me
    partner = me + 1 - 2 * (me % 2)
    across = (me + 2) % GROUP
    beyond = (partner + 2) % GROUP
    behind = block >= GROUP
    ahead = block + GROUP < count
    last = GROUP - 1
    first_chip = me < 2

    def columns_of(head):
        return pl.ds(pl.multiple_of(head * HD, HD), HD)

    def remote(src, dst, sender, recv, target):
        return pltpu.make_async_remote_copy(
            src_ref=src, dst_ref=dst, send_sem=sender, recv_sem=recv,
            device_id=target, device_id_type=pl.DeviceIdType.MESH,
        )

    def landed(ref, sem):
        remote(ref, ref, send.at[0], sem, {"tm": block}).wait_recv()

    def sent(ref, sem):
        remote(ref, ref, sem, out_sem, {"tm": block}).wait_send()

    if tiles == 2:
        sides = [(tile >= 1, 1 - 2 * tile, None)]
    elif tiles > 2:
        sides = [(None, -1, tile >= 1), (None, 1, tile + 1 < tiles)]
    else:
        sides = []

    def maybe(condition, action):
        if condition is None:
            action()
        else:
            pl.when(condition)(action)

    barrier = pltpu.get_barrier_semaphore()
    expected = jnp.int32(GROUP - 1)

    def greet(target):
        pl.semaphore_signal(barrier, inc=1, device_id=target, device_id_type=pl.DeviceIdType.MESH)

    for role in (across, beyond, partner):
        greet({"tm": base + role})
    for _, step, there in sides:
        maybe(there, lambda: greet({"tile": tile + step}))
        expected += 1 if there is None else there.astype(jnp.int32)
    for there, step in ((behind, -GROUP), (ahead, GROUP)):
        pl.when(there)(lambda: greet({"tm": block + step}))
        expected += there.astype(jnp.int32)

    pltpu.make_async_copy(lists_hbm, lists_ref, small_sem.at[0]).start()
    pltpu.make_async_copy(halo_hbm, halo_ref, small_sem.at[1]).start()

    def spots(h):
        return ((k_ref, kv.at[me, h, 0]), (v_ref, kv.at[me, h, 1]), (q_ref, qs.at[me, h]))

    def fetch(h, carry):
        for ref, spot in spots(h):
            pltpu.make_async_copy(ref.at[:, columns_of(me * share + h)], spot, local_sem).start()
        return carry

    lax.fori_loop(0, share, fetch, 0)

    pltpu.make_async_copy(lists_hbm, lists_ref, small_sem.at[0]).wait()
    pltpu.make_async_copy(halo_hbm, halo_ref, small_sem.at[1]).wait()
    row = lax.broadcasted_iota(jnp.int32, (ROWS, tokens), 0)
    mine = jnp.where(row == slots, halo_ref[0, 0, 0], -1)
    for n in range(slots):
        mine = jnp.where(row == n, lists_ref[0, 0, n], mine)
    info[me] = mine

    pl.semaphore_wait(barrier, expected)

    def give(role, h, pairs, sem):
        for ref, spot in pairs:
            kind = Q_SENT if ref is q_ref else KV_SENT
            remote(ref.at[:, columns_of(role * share + h)], spot, send.at[kind], sem,
                   {"tm": base + role}).start()

    def give_keys(h):
        for role in (across, beyond):
            give(role, h, spots(h)[:2], kv_sem.at[h])

    def give_queries(h):
        for role in (across, beyond):
            give(role, h, spots(h)[2:], q_sem.at[h])

    def to_sides(role, kind, h):
        for at, (_, step, there) in enumerate(sides):
            other = len(sides) - 1 - at
            maybe(there, lambda: remote(
                kv.at[role, h], side.at[other, role, h], side_send.at[at],
                side_sem.at[other, kind, h], {"tile": tile + step}).start())

    def to_next(role, h):
        @pl.when(both(role == last, ahead))
        def _():
            remote(kv.at[role, h], past.at[h], send.at[PAST_SENT], past_sem.at[h],
                   {"tm": block + GROUP}).start()

    def to_before(role, h):
        @pl.when(behind)
        def _():
            remote(qs.at[role, h], ask.at[role, h], send.at[ASK_SENT], ask_sem.at[h],
                   {"tm": block - GROUP}).start()

    def near_z(h):
        for role in (me, partner):
            to_before(role, h)
            to_next(role, h)

    for role in (across, beyond, partner):
        remote(info.at[me], info.at[me], send.at[INFO_SENT], info_sem.at[0],
               {"tm": base + role}).start()
    give_keys(0)
    pltpu.make_async_copy(kv.at[me], kv.at[me], local_sem).wait()
    pltpu.make_async_copy(qs.at[me], qs.at[me], local_sem).wait()
    to_sides(me, MINE, 0)
    for h in range(min(3, share)):
        give_queries(h)
    give(partner, 0, spots(0), near_sem.at[0])

    def give_rest(h, carry):
        give(partner, h, spots(h), near_sem.at[1])
        return carry

    def give_far(h, carry):
        give_keys(h)
        pl.when(h + 2 < share)(lambda: give_queries(h + 2))
        return carry

    lax.fori_loop(1, share, give_rest, 0)
    lax.fori_loop(1, share, give_far, 0)
    landed(res.at[pl.ds(0, 3), 0], near_sem.at[0])
    to_sides(partner, NEAR, 0)
    near_z(0)

    landed(info.at[pl.ds(0, GROUP - 1)], info_sem.at[0])

    @pl.when(behind)
    def _():
        remote(info.at[pl.ds(0, GROUP)], info.at[pl.ds(GROUP, GROUP)], send.at[ASKED_SENT],
               info_sem.at[1], {"tm": block - GROUP}).start()

    landed(res.at[pl.ds(0, 3), pl.ds(0, share - 1)], near_sem.at[1])

    def near_sides(h):
        to_sides(partner, NEAR, h)
        to_sides(me, MINE, h)

    near_sides(1)

    @pl.when(jnp.logical_not(behind))
    def _():
        past[...] = jnp.zeros(past.shape, past.dtype)
        back[...] = jnp.zeros(back.shape, back.dtype)
        back_stat[...] = jnp.full(back_stat.shape, LOW, back_stat.dtype)

    for at, (_, _, there) in enumerate(sides):
        if there is not None:

            @pl.when(jnp.logical_not(there))
            def _():
                side[at] = jnp.zeros(side.shape[1:], side.dtype)

    def spread(at, number):
        out = jnp.full((ROWS, tokens), LOW, jnp.float32)
        for d in range(1, WIN + 1):
            wanted = jnp.where(number >= d, number - d, -2)
            hit = info[at, 0:1, :] == wanted
            for n in range(1, slots):
                hit = jnp.logical_or(hit, info[at, n : n + 1, :] == wanted)
            out = jnp.where(jnp.logical_and(row == d, hit), 0.0, out)
        far[at] = out

    query = lax.broadcasted_iota(jnp.int32, (tokens, tokens), 0) // (rows * columns)
    key = lax.broadcasted_iota(jnp.int32, (tokens, tokens), 1)
    causal = key // (rows * columns) <= query
    bias[0] = jnp.where(causal, 0.0, LOW)
    key_row = (lax.broadcasted_iota(jnp.int32, (1, tokens), 1) // columns) % rows
    for role in range(GROUP):
        spread(role, base + role)
        reach = info[role, slots : slots + 1, :]
        above = jnp.where(key_row >= rows - reach, 0.0, LOW)
        below = jnp.where(key_row < reach, 0.0, LOW)
        for at, (upper, step, there) in enumerate(sides):
            if upper is not None:
                edge = jnp.where(upper, above, below)
            else:
                edge = jnp.where(there, above if step < 0 else below, LOW)
            bias[1 + role * len(sides) + at] = jnp.where(causal, edge, LOW)

    @pl.when(ahead)
    def _():
        landed(info.at[pl.ds(GROUP, GROUP)], info_sem.at[1])

        for role in range(GROUP):
            spread(GROUP + role, base + GROUP + role)

    def attend(query_part, parts):
        scores = []
        most = None
        for pair, shift in parts:
            s = lax.dot_general(query_part, pair[0], (((1,), (1,)), ((), ())),
                                preferred_element_type=jnp.float32) + shift
            most = s if most is None else jnp.maximum(most, s)
            scores.append(s)
        top = jnp.max(most, axis=1, keepdims=True) * SCALE
        total = None
        numerator = None
        for s, (pair, _) in zip(scores, parts):
            w = jnp.exp2(s * SCALE - top)
            total = w if total is None else total + w
            term = jnp.dot(w.astype(jnp.bfloat16), pair[1], preferred_element_type=jnp.float32)
            numerator = term if numerator is None else numerator + term
        return numerator, jnp.sum(total, axis=1, keepdims=True), top

    def distant(at, d):
        return far[at, d : d + 1, :]

    def visit(role, h):
        parts = []
        for other in range(GROUP):
            d = role + GROUP - other
            if d <= WIN:
                parts.append((kv.at[other, h], distant(GROUP + role, d)))
        if role + 1 + GROUP <= WIN:
            pl.when(behind)(lambda: landed(past.at[h], past_sem.at[h]))
            parts.append((past.at[h], distant(GROUP + role, role + 1 + GROUP)))
        numerator, total, top = attend(ask[role, h], parts)
        part[role, h] = (numerator / total).astype(part.dtype)
        level = jnp.broadcast_to(top + jnp.log2(total), (tokens, HD))
        stat[role, h] = jnp.transpose(level)[0:1, :]
        kind = role // 2
        remote(part.at[role, h], back.at[role, h], send.at[BACK_SENT + kind], back_sem.at[kind, h],
               {"tm": block + GROUP}).start()
        remote(stat.at[role, h], back_stat.at[role, h], send.at[STAT_SENT + kind],
               stat_sem.at[kind, h], {"tm": block + GROUP}).start()

    two = pl.ds(0, 2)

    def returned(kind, h):
        landed(back.at[two, h], back_sem.at[kind, h])
        landed(back_stat.at[two, h], stat_sem.at[kind, h])

    def sides_here(kind, h):
        roles = {FAR: two, NEAR: partner, MINE: me}[kind]
        for at, (_, _, there) in enumerate(sides):
            maybe(there, lambda: landed(side.at[at, roles, h], side_sem.at[at, kind, h]))

    def merge(one, other):
        peak = jnp.maximum(one[2], other[2])
        ours, theirs = jnp.exp2(one[2] - peak), jnp.exp2(other[2] - peak)
        return one[0] * ours + other[0] * theirs, one[1] * ours + other[1] * theirs, peak

    def unit(role, h, between=None):
        parts = [(kv.at[role, h], bias[0])]
        for other in range(role):
            parts.append((kv.at[other, h], distant(role, role - other)))
        margins = [(side.at[at, role, h], bias[1 + role * len(sides) + at]) for at in range(len(sides))]
        level = jnp.transpose(jnp.broadcast_to(back_stat[role, h], (HD, tokens)))
        so_far = (back[role, h].astype(jnp.float32), 1.0, level)
        if between is None:
            parts += margins
        so_far = merge(so_far, attend(qs[role, h], parts))
        if between is not None:
            between()
            if margins:
                so_far = merge(so_far, attend(qs[role, h], margins))
        numerator, total, _ = so_far
        res[role, h] = (numerator / total).astype(res.dtype)
        place = columns_of(me * share + h)

        @pl.when(me == role)
        def _():
            out_ref[:, place] = res[role, h]

        @pl.when(me != role)
        def _():
            remote(res.at[role, h], out_ref.at[:, place], send.at[RES_SENT], out_sem,
                   {"tm": base + role}).start()

    def rest(t):
        h = t - 1

        def one(n, carry):
            k = jnp.where(n == 2, -1, n - (n > 2).astype(jnp.int32))
            turn = jnp.where(k == 0, across, jnp.where(k == 1, beyond, jnp.where(k == 2, partner, me)))
            final = both(k == 3, t == share)

            @pl.when(t >= 1)
            def _():
                pl.when(both(k == 0, behind))(lambda: returned(1 - me // 2, h))
                pl.when(both(k == 2, behind))(lambda: returned(me // 2, h))
                pl.when(k == 0)(lambda: sides_here(FAR, h))
                pl.when(k == 2)(lambda: sides_here(NEAR, h))
                pl.when(both(k == 3, t < share))(lambda: sides_here(MINE, h))

            pl.when(both(k == 3, t + 2 == share))(lambda: keys_here(t + 1))
            for role in range(GROUP):
                pl.when(both(k >= 0, t >= 1, turn == role, jnp.logical_not(final)))(
                    lambda: unit(role, h))
                pl.when(both(final, turn == role))(
                    lambda: unit(role, h, lambda: sides_here(MINE, h)))

            pl.when(both(k < 0, t < share, ahead, first_chip))(lambda: visit(0, t))
            pl.when(both(k < 0, t < share, ahead, jnp.logical_not(first_chip)))(lambda: visit(last, t))
            return carry

        lax.fori_loop(0, GROUP + 1, one, 0)

    def keys_here(h):
        landed(kv.at[two, h], kv_sem.at[h])
        for role in (across, beyond):
            to_sides(role, FAR, h)
            to_next(role, h)

    def query_here(h):
        landed(qs.at[two, h], q_sem.at[h])
        for role in (across, beyond):
            to_before(role, h)

    def step(t, carry):
        @pl.when(t < share)
        def _():
            pl.when(t + 1 < share)(lambda: keys_here(t))
            pl.when(t + 3 < share)(lambda: to_sides(partner, NEAR, t + 2))
            pl.when(both(t == 0, t + 3 < share))(lambda: to_sides(me, MINE, t + 2))
            pl.when(both(t >= 2, t + 2 < share))(lambda: to_sides(me, MINE, t + 1))
            pl.when(both(t + 1 == share, share > 2))(lambda: near_sides(t))
            pl.when(t == 0)(lambda: query_here(t))

            @pl.when(t + 1 < share)
            def _():
                query_here(t + 1)
                pl.when(t == 0)(lambda: near_z(t + 1))
                pl.when(t + 2 < share)(lambda: near_z(t + 2))

            @pl.when(ahead)
            def _():
                landed(ask.at[:, t], ask_sem.at[t])

                @pl.when(first_chip)
                def _():
                    for role in (2, 3, 1):
                        visit(role, t)

                @pl.when(jnp.logical_not(first_chip))
                def _():
                    for role in (1, 0, 2):
                        visit(role, t)

            pl.when(both(behind, jnp.logical_not(ahead)))(lambda: landed(past.at[t], past_sem.at[t]))

        rest(t)
        return carry

    lax.fori_loop(0, share + 1, step, 0)

    peers = pl.ds(0, GROUP - 1)
    landed(res.at[peers], out_sem)
    sent(res.at[peers], send.at[RES_SENT])
    sent(info.at[peers], send.at[INFO_SENT])
    sent(qs.at[peers], send.at[Q_SENT])
    sent(kv.at[peers], send.at[KV_SENT])
    for at, (_, _, there) in enumerate(sides):
        maybe(there, lambda: sent(side.at[at], side_send.at[at]))

    @pl.when(ahead)
    def _():
        sent(past, send.at[PAST_SENT])
        for kind in range(2):
            sent(back.at[two], send.at[BACK_SENT + kind])
            sent(back_stat.at[two], send.at[STAT_SENT + kind])

    @pl.when(behind)
    def _():
        sent(ask, send.at[ASK_SENT])
        sent(info.at[pl.ds(0, GROUP)], send.at[ASKED_SENT])


def local(count, tiles, queries, keys, values, neighbours, halo_rows):
    frames, rows, columns, channels = queries.shape
    tokens = frames * rows * columns
    heads = channels // HD
    share = heads // GROUP
    assert rows == HMAX and count % GROUP == 0 and heads % GROUP == 0
    sides = min(2, tiles - 1)
    flat = (tokens, channels)
    piece = (tokens, HD)
    anywhere = pl.BlockSpec(memory_space=pltpu.HBM)
    dma = pltpu.SemaphoreType.DMA

    def vmem(*size, dtype=jnp.bfloat16):
        return pltpu.VMEM(size, dtype)

    out = pl.pallas_call(
        functools.partial(kernel, count, tiles, (frames, rows, columns)),
        out_shape=pltpu.VMEM(flat, jnp.bfloat16),
        in_specs=[anywhere] * 5,
        out_specs=pl.BlockSpec(memory_space=pltpu.VMEM),
        scratch_shapes=[
            pltpu.SMEM(neighbours.shape, jnp.int32),
            pltpu.SMEM((1, 1, 1), jnp.int32),
            vmem(GROUP, share, *piece),
            vmem(GROUP, share, 2, *piece),
            vmem(max(1, sides), GROUP, share, 2, *piece),
            vmem(share, 2, *piece),
            vmem(GROUP, share, *piece),
            vmem(GROUP, share, *piece),
            vmem(GROUP, share, 1, tokens, dtype=jnp.float32),
            vmem(GROUP, share, *piece),
            vmem(GROUP, share, 1, tokens, dtype=jnp.float32),
            vmem(GROUP, share, *piece),
            vmem(2 * GROUP, ROWS, tokens, dtype=jnp.int32),
            vmem(2 * GROUP, ROWS, tokens, dtype=jnp.float32),
            vmem(1 + GROUP * sides, tokens, tokens, dtype=jnp.float32),
            dma((2,)),
            dma((KINDS,)),
            dma((max(1, sides),)),
            dma,
            dma((2,)),
            dma((share,)),
            dma((share,)),
            dma((max(1, sides), 3, share)),
            dma((share,)),
            dma((share,)),
            dma((2, share)),
            dma((2, share)),
            dma,
            dma((2,)),
        ],
        compiler_params=pltpu.CompilerParams(
            collective_id=0, has_side_effects=True, vmem_limit_bytes=56 * 1024 * 1024
        ),
    )(
        neighbours,
        halo_rows.reshape(1, 1, 1),
        queries.reshape(flat),
        keys.reshape(flat),
        values.reshape(flat),
    )
    return out.reshape(queries.shape)


def solution(mesh):
    return jax.shard_map(
        functools.partial(local, mesh.shape["tm"], mesh.shape["tile"]),
        mesh=mesh,
        in_specs=(
            P("tm", "tile", None, None),
            P("tm", "tile", None, None),
            P("tm", "tile", None, None),
            P("tm", "tile", None),
            P("tm", "tile"),
        ),
        out_specs=P("tm", "tile", None, None),
        check_vma=False,
    )
```

```python
import functools
import math

import jax
import jax.numpy as jnp
from jax import lax
from jax.experimental import pallas as pl
from jax.experimental.pallas import tpu as pltpu
from jax.sharding import PartitionSpec as P

HD = 128
HMAX = 2
WIN = 5
GROUP = 4
FAR, NEAR, MINE = range(3)
Q_SENT, KV_SENT, RES_SENT, INFO_SENT, ASK_SENT, ASKED_SENT, PAST_SENT, BACK_SENT = range(8)
STAT_SENT = BACK_SENT + 2
KINDS = STAT_SENT + 2
ROWS = 8
LOW = -1e9
SCALE = math.log2(math.e) / math.sqrt(HD)


def both(*terms):
    out = terms[0]
    for term in terms[1:]:
        out = jnp.logical_and(out, term)
    return out


def kernel(count, tiles, shape, lists_hbm, halo_hbm, q_ref, k_ref, v_ref, out_ref,
           lists_ref, halo_ref,
           qs, kv, side, past, ask, part, stat, back, back_stat, res, info, far, bias,
           small_sem, send, side_send, local_sem, near_sem, q_sem, kv_sem, side_sem, past_sem, ask_sem,
           back_sem, stat_sem, out_sem, info_sem):
    frames, rows, columns = shape
    tokens = frames * rows * columns
    share = kv.shape[1]
    slots = lists_ref.shape[2]
    block = lax.axis_index("tm")
    tile = lax.axis_index("tile")
    me = block % GROUP
    base = block - me
    partner = me + 1 - 2 * (me % 2)
    across = (me + 2) % GROUP
    beyond = (partner + 2) % GROUP
    behind = block >= GROUP
    ahead = block + GROUP < count
    last = GROUP - 1
    first_chip = me < 2

    def columns_of(head):
        return pl.ds(pl.multiple_of(head * HD, HD), HD)

    def remote(src, dst, sender, recv, target):
        return pltpu.make_async_remote_copy(
            src_ref=src, dst_ref=dst, send_sem=sender, recv_sem=recv,
            device_id=target, device_id_type=pl.DeviceIdType.MESH,
        )

    def landed(ref, sem):
        remote(ref, ref, send.at[0], sem, {"tm": block}).wait_recv()

    def sent(ref, sem):
        remote(ref, ref, sem, out_sem, {"tm": block}).wait_send()

    if tiles == 2:
        sides = [(tile >= 1, 1 - 2 * tile, None)]
    elif tiles > 2:
        sides = [(None, -1, tile >= 1), (None, 1, tile + 1 < tiles)]
    else:
        sides = []

    def maybe(condition, action):
        if condition is None:
            action()
        else:
            pl.when(condition)(action)

    barrier = pltpu.get_barrier_semaphore()
    expected = jnp.int32(GROUP - 1)

    def greet(target):
        pl.semaphore_signal(barrier, inc=1, device_id=target, device_id_type=pl.DeviceIdType.MESH)

    for role in (across, beyond, partner):
        greet({"tm": base + role})
    for _, step, there in sides:
        maybe(there, lambda: greet({"tile": tile + step}))
        expected += 1 if there is None else there.astype(jnp.int32)
    for there, step in ((behind, -GROUP), (ahead, GROUP)):
        pl.when(there)(lambda: greet({"tm": block + step}))
        expected += there.astype(jnp.int32)

    pltpu.make_async_copy(lists_hbm, lists_ref, small_sem.at[0]).start()
    pltpu.make_async_copy(halo_hbm, halo_ref, small_sem.at[1]).start()

    def spots(h):
        return ((k_ref, kv.at[me, h, 0]), (v_ref, kv.at[me, h, 1]), (q_ref, qs.at[me, h]))

    def fetch(h, carry):
        for ref, spot in spots(h):
            pltpu.make_async_copy(ref.at[:, columns_of(me * share + h)], spot, local_sem).start()
        return carry

    lax.fori_loop(0, share, fetch, 0)

    pltpu.make_async_copy(lists_hbm, lists_ref, small_sem.at[0]).wait()
    pltpu.make_async_copy(halo_hbm, halo_ref, small_sem.at[1]).wait()
    row = lax.broadcasted_iota(jnp.int32, (ROWS, tokens), 0)
    mine = jnp.where(row == slots, halo_ref[0, 0, 0], -1)
    for n in range(slots):
        mine = jnp.where(row == n, lists_ref[0, 0, n], mine)
    info[me] = mine

    pl.semaphore_wait(barrier, expected)

    def give(role, h, pairs, sem):
        for ref, spot in pairs:
            kind = Q_SENT if ref is q_ref else KV_SENT
            remote(ref.at[:, columns_of(role * share + h)], spot, send.at[kind], sem,
                   {"tm": base + role}).start()

    def give_keys(h):
        for role in (across, beyond):
            give(role, h, spots(h)[:2], kv_sem.at[h])

    def give_queries(h):
        for role in (across, beyond):
            give(role, h, spots(h)[2:], q_sem.at[h])

    def to_sides(role, kind, h):
        for at, (_, step, there) in enumerate(sides):
            other = len(sides) - 1 - at
            maybe(there, lambda: remote(
                kv.at[role, h], side.at[other, role, h], side_send.at[at],
                side_sem.at[other, kind, h], {"tile": tile + step}).start())

    def to_next(role, h):
        @pl.when(both(role == last, ahead))
        def _():
            remote(kv.at[role, h], past.at[h], send.at[PAST_SENT], past_sem.at[h],
                   {"tm": block + GROUP}).start()

    def to_before(role, h):
        @pl.when(behind)
        def _():
            remote(qs.at[role, h], ask.at[role, h], send.at[ASK_SENT], ask_sem.at[h],
                   {"tm": block - GROUP}).start()

    def near_z(h):
        for role in (me, partner):
            to_before(role, h)
            to_next(role, h)

    for role in (across, beyond, partner):
        remote(info.at[me], info.at[me], send.at[INFO_SENT], info_sem.at[0],
               {"tm": base + role}).start()
    give_keys(0)
    pltpu.make_async_copy(kv.at[me], kv.at[me], local_sem).wait()
    pltpu.make_async_copy(qs.at[me], qs.at[me], local_sem).wait()
    to_sides(me, MINE, 0)
    for h in range(min(3, share)):
        give_queries(h)
    give(partner, 0, spots(0), near_sem.at[0])

    def give_rest(h, carry):
        give(partner, h, spots(h), near_sem.at[1])
        return carry

    def give_far(h, carry):
        give_keys(h)
        pl.when(h + 2 < share)(lambda: give_queries(h + 2))
        return carry

    lax.fori_loop(1, share, give_rest, 0)
    lax.fori_loop(1, share, give_far, 0)
    landed(res.at[pl.ds(0, 3), 0], near_sem.at[0])
    to_sides(partner, NEAR, 0)
    near_z(0)

    landed(info.at[pl.ds(0, GROUP - 1)], info_sem.at[0])

    @pl.when(behind)
    def _():
        remote(info.at[pl.ds(0, GROUP)], info.at[pl.ds(GROUP, GROUP)], send.at[ASKED_SENT],
               info_sem.at[1], {"tm": block - GROUP}).start()

    landed(res.at[pl.ds(0, 3), pl.ds(0, share - 1)], near_sem.at[1])

    def near_sides(h):
        to_sides(partner, NEAR, h)
        to_sides(me, MINE, h)

    near_sides(1)

    @pl.when(jnp.logical_not(behind))
    def _():
        past[...] = jnp.zeros(past.shape, past.dtype)
        back[...] = jnp.zeros(back.shape, back.dtype)
        back_stat[...] = jnp.full(back_stat.shape, LOW, back_stat.dtype)

    for at, (_, _, there) in enumerate(sides):
        if there is not None:

            @pl.when(jnp.logical_not(there))
            def _():
                side[at] = jnp.zeros(side.shape[1:], side.dtype)

    def spread(at, number):
        out = jnp.full((ROWS, tokens), LOW, jnp.float32)
        for d in range(1, WIN + 1):
            wanted = jnp.where(number >= d, number - d, -2)
            hit = info[at, 0:1, :] == wanted
            for n in range(1, slots):
                hit = jnp.logical_or(hit, info[at, n : n + 1, :] == wanted)
            out = jnp.where(jnp.logical_and(row == d, hit), 0.0, out)
        far[at] = out

    query = lax.broadcasted_iota(jnp.int32, (tokens, tokens), 0) // (rows * columns)
    key = lax.broadcasted_iota(jnp.int32, (tokens, tokens), 1)
    causal = key // (rows * columns) <= query
    bias[0] = jnp.where(causal, 0.0, LOW)
    key_row = (lax.broadcasted_iota(jnp.int32, (1, tokens), 1) // columns) % rows
    for role in range(GROUP):
        spread(role, base + role)
        reach = info[role, slots : slots + 1, :]
        above = jnp.where(key_row >= rows - reach, 0.0, LOW)
        below = jnp.where(key_row < reach, 0.0, LOW)
        for at, (upper, step, there) in enumerate(sides):
            if upper is not None:
                edge = jnp.where(upper, above, below)
            else:
                edge = jnp.where(there, above if step < 0 else below, LOW)
            bias[1 + role * len(sides) + at] = jnp.where(causal, edge, LOW)

    @pl.when(ahead)
    def _():
        landed(info.at[pl.ds(GROUP, GROUP)], info_sem.at[1])

        for role in range(GROUP):
            spread(GROUP + role, base + GROUP + role)

    def attend(query_part, parts):
        scores = []
        most = None
        for pair, shift in parts:
            s = lax.dot_general(query_part, pair[0], (((1,), (1,)), ((), ())),
                                preferred_element_type=jnp.float32) + shift
            most = s if most is None else jnp.maximum(most, s)
            scores.append(s)
        top = jnp.max(most, axis=1, keepdims=True) * SCALE
        total = None
        numerator = None
        for s, (pair, _) in zip(scores, parts):
            w = jnp.exp2(s * SCALE - top)
            total = w if total is None else total + w
            term = jnp.dot(w.astype(jnp.bfloat16), pair[1], preferred_element_type=jnp.float32)
            numerator = term if numerator is None else numerator + term
        return numerator, jnp.sum(total, axis=1, keepdims=True), top

    def distant(at, d):
        return far[at, d : d + 1, :]

    def visit(role, h):
        parts = []
        for other in range(GROUP):
            d = role + GROUP - other
            if d <= WIN:
                parts.append((kv.at[other, h], distant(GROUP + role, d)))
        if role + 1 + GROUP <= WIN:
            pl.when(behind)(lambda: landed(past.at[h], past_sem.at[h]))
            parts.append((past.at[h], distant(GROUP + role, role + 1 + GROUP)))
        numerator, total, top = attend(ask[role, h], parts)
        part[role, h] = (numerator / total).astype(part.dtype)
        level = jnp.broadcast_to(top + jnp.log2(total), (tokens, HD))
        stat[role, h] = jnp.transpose(level)[0:1, :]
        kind = role // 2
        remote(part.at[role, h], back.at[role, h], send.at[BACK_SENT + kind], back_sem.at[kind, h],
               {"tm": block + GROUP}).start()
        remote(stat.at[role, h], back_stat.at[role, h], send.at[STAT_SENT + kind],
               stat_sem.at[kind, h], {"tm": block + GROUP}).start()

    two = pl.ds(0, 2)

    def returned(kind, h):
        landed(back.at[two, h], back_sem.at[kind, h])
        landed(back_stat.at[two, h], stat_sem.at[kind, h])

    def sides_here(kind, h):
        roles = {FAR: two, NEAR: partner, MINE: me}[kind]
        for at, (_, _, there) in enumerate(sides):
            maybe(there, lambda: landed(side.at[at, roles, h], side_sem.at[at, kind, h]))

    def merge(one, other):
        peak = jnp.maximum(one[2], other[2])
        ours, theirs = jnp.exp2(one[2] - peak), jnp.exp2(other[2] - peak)
        return one[0] * ours + other[0] * theirs, one[1] * ours + other[1] * theirs, peak

    def unit(role, h, between=None):
        parts = [(kv.at[role, h], bias[0])]
        for other in range(role):
            parts.append((kv.at[other, h], distant(role, role - other)))
        margins = [(side.at[at, role, h], bias[1 + role * len(sides) + at]) for at in range(len(sides))]
        level = jnp.transpose(jnp.broadcast_to(back_stat[role, h], (HD, tokens)))
        so_far = (back[role, h].astype(jnp.float32), 1.0, level)
        if between is None:
            parts += margins
        so_far = merge(so_far, attend(qs[role, h], parts))
        if between is not None:
            between()
            if margins:
                so_far = merge(so_far, attend(qs[role, h], margins))
        numerator, total, _ = so_far
        res[role, h] = (numerator / total).astype(res.dtype)
        place = columns_of(me * share + h)

        @pl.when(me == role)
        def _():
            out_ref[:, place] = res[role, h]

        @pl.when(me != role)
        def _():
            remote(res.at[role, h], out_ref.at[:, place], send.at[RES_SENT], out_sem,
                   {"tm": base + role}).start()

    def rest(t):
        h = t - 1

        def one(n, carry):
            k = jnp.where(n == 2, -1, n - (n > 2).astype(jnp.int32))
            turn = jnp.where(k == 0, across, jnp.where(k == 1, beyond, jnp.where(k == 2, partner, me)))
            final = both(k == 3, t == share)

            @pl.when(t >= 1)
            def _():
                pl.when(both(k == 0, behind))(lambda: returned(1 - me // 2, h))
                pl.when(both(k == 2, behind))(lambda: returned(me // 2, h))
                pl.when(k == 0)(lambda: sides_here(FAR, h))
                pl.when(k == 2)(lambda: sides_here(NEAR, h))
                pl.when(both(k == 3, t < share))(lambda: sides_here(MINE, h))

            pl.when(both(k == 3, t + 2 == share))(lambda: keys_here(t + 1))
            for role in range(GROUP):
                pl.when(both(k >= 0, t >= 1, turn == role, jnp.logical_not(final)))(
                    lambda: unit(role, h))
                pl.when(both(final, turn == role))(
                    lambda: unit(role, h, lambda: sides_here(MINE, h)))

            pl.when(both(k < 0, t < share, ahead, first_chip))(lambda: visit(0, t))
            pl.when(both(k < 0, t < share, ahead, jnp.logical_not(first_chip)))(lambda: visit(last, t))
            return carry

        lax.fori_loop(0, GROUP + 1, one, 0)

    def keys_here(h):
        landed(kv.at[two, h], kv_sem.at[h])
        for role in (across, beyond):
            to_sides(role, FAR, h)
            to_next(role, h)

    def query_here(h):
        landed(qs.at[two, h], q_sem.at[h])
        for role in (across, beyond):
            to_before(role, h)

    def step(t, carry):
        @pl.when(t < share)
        def _():
            pl.when(t + 1 < share)(lambda: keys_here(t))
            pl.when(t + 3 < share)(lambda: to_sides(partner, NEAR, t + 2))
            pl.when(both(t == 0, t + 3 < share))(lambda: to_sides(me, MINE, t + 2))
            pl.when(both(t >= 2, t + 2 < share))(lambda: to_sides(me, MINE, t + 1))
            pl.when(both(t + 1 == share, share > 2))(lambda: near_sides(t))
            pl.when(t == 0)(lambda: query_here(t))

            @pl.when(t + 1 < share)
            def _():
                query_here(t + 1)
                pl.when(t == 0)(lambda: near_z(t + 1))
                pl.when(t + 2 < share)(lambda: near_z(t + 2))

            @pl.when(ahead)
            def _():
                landed(ask.at[:, t], ask_sem.at[t])

                @pl.when(first_chip)
                def _():
                    for role in (2, 3, 1):
                        visit(role, t)

                @pl.when(jnp.logical_not(first_chip))
                def _():
                    for role in (1, 0, 2):
                        visit(role, t)

            pl.when(both(behind, jnp.logical_not(ahead)))(lambda: landed(past.at[t], past_sem.at[t]))

        rest(t)
        return carry

    lax.fori_loop(0, share + 1, step, 0)

    peers = pl.ds(0, GROUP - 1)
    landed(res.at[peers], out_sem)
    sent(res.at[peers], send.at[RES_SENT])
    sent(info.at[peers], send.at[INFO_SENT])
    sent(qs.at[peers], send.at[Q_SENT])
    sent(kv.at[peers], send.at[KV_SENT])
    for at, (_, _, there) in enumerate(sides):
        maybe(there, lambda: sent(side.at[at], side_send.at[at]))

    @pl.when(ahead)
    def _():
        sent(past, send.at[PAST_SENT])
        for kind in range(2):
            sent(back.at[two], send.at[BACK_SENT + kind])
            sent(back_stat.at[two], send.at[STAT_SENT + kind])

    @pl.when(behind)
    def _():
        sent(ask, send.at[ASK_SENT])
        sent(info.at[pl.ds(0, GROUP)], send.at[ASKED_SENT])


def local(count, tiles, queries, keys, values, neighbours, halo_rows):
    frames, rows, columns, channels = queries.shape
    tokens = frames * rows * columns
    heads = channels // HD
    share = heads // GROUP
    assert rows == HMAX and count % GROUP == 0 and heads % GROUP == 0
    sides = min(2, tiles - 1)
    flat = (tokens, channels)
    piece = (tokens, HD)
    anywhere = pl.BlockSpec(memory_space=pltpu.HBM)
    dma = pltpu.SemaphoreType.DMA

    def vmem(*size, dtype=jnp.bfloat16):
        return pltpu.VMEM(size, dtype)

    out = pl.pallas_call(
        functools.partial(kernel, count, tiles, (frames, rows, columns)),
        out_shape=pltpu.VMEM(flat, jnp.bfloat16),
        in_specs=[anywhere] * 5,
        out_specs=pl.BlockSpec(memory_space=pltpu.VMEM),
        scratch_shapes=[
            pltpu.SMEM(neighbours.shape, jnp.int32),
            pltpu.SMEM((1, 1, 1), jnp.int32),
            vmem(GROUP, share, *piece),
            vmem(GROUP, share, 2, *piece),
            vmem(max(1, sides), GROUP, share, 2, *piece),
            vmem(share, 2, *piece),
            vmem(GROUP, share, *piece),
            vmem(GROUP, share, *piece),
            vmem(GROUP, share, 1, tokens, dtype=jnp.float32),
            vmem(GROUP, share, *piece),
            vmem(GROUP, share, 1, tokens, dtype=jnp.float32),
            vmem(GROUP, share, *piece),
            vmem(2 * GROUP, ROWS, tokens, dtype=jnp.int32),
            vmem(2 * GROUP, ROWS, tokens, dtype=jnp.float32),
            vmem(1 + GROUP * sides, tokens, tokens, dtype=jnp.float32),
            dma((2,)),
            dma((KINDS,)),
            dma((max(1, sides),)),
            dma,
            dma((2,)),
            dma((share,)),
            dma((share,)),
            dma((max(1, sides), 3, share)),
            dma((share,)),
            dma((share,)),
            dma((2, share)),
            dma((2, share)),
            dma,
            dma((2,)),
        ],
        compiler_params=pltpu.CompilerParams(
            collective_id=0, has_side_effects=True, vmem_limit_bytes=56 * 1024 * 1024
        ),
    )(
        neighbours,
        halo_rows.reshape(1, 1, 1),
        queries.reshape(flat),
        keys.reshape(flat),
        values.reshape(flat),
    )
    return out.reshape(queries.shape)


def solution(mesh):
    return jax.shard_map(
        functools.partial(local, mesh.shape["tm"], mesh.shape["tile"]),
        mesh=mesh,
        in_specs=(
            P("tm", "tile", None, None),
            P("tm", "tile", None, None),
            P("tm", "tile", None, None),
            P("tm", "tile", None),
            P("tm", "tile"),
        ),
        out_specs=P("tm", "tile", None, None),
        check_vma=False,
    )
```

```python
import functools
import math

import jax
import jax.numpy as jnp
from jax import lax
from jax.experimental import pallas as pl
from jax.experimental.pallas import tpu as pltpu
from jax.sharding import PartitionSpec as P

HD = 128
HMAX = 2
WIN = 5
GROUP = 4
FAR, NEAR, MINE = range(3)
Q_SENT, KV_SENT, RES_SENT, INFO_SENT, ASK_SENT, ASKED_SENT, PAST_SENT, BACK_SENT = range(8)
STAT_SENT = BACK_SENT + 2
KINDS = STAT_SENT + 2
ROWS = 8
LOW = -1e9
SCALE = math.log2(math.e) / math.sqrt(HD)


def both(*terms):
    out = terms[0]
    for term in terms[1:]:
        out = jnp.logical_and(out, term)
    return out


def kernel(count, tiles, shape, lists_hbm, halo_hbm, q_ref, k_ref, v_ref, out_ref,
           lists_ref, halo_ref,
           qs, kv, side, past, ask, part, stat, back, back_stat, res, info, far, bias,
           stage, stage_sem, small_sem, send, side_send, local_sem, near_sem, q_sem, kv_sem, side_sem, past_sem, ask_sem,
           back_sem, stat_sem, out_sem, info_sem):
    frames, rows, columns = shape
    tokens = frames * rows * columns
    share = kv.shape[1]
    slots = lists_ref.shape[2]
    block = lax.axis_index("tm")
    tile = lax.axis_index("tile")
    me = block % GROUP
    base = block - me
    partner = me + 1 - 2 * (me % 2)
    across = (me + 2) % GROUP
    beyond = (partner + 2) % GROUP
    behind = block >= GROUP
    ahead = block + GROUP < count
    last = GROUP - 1
    first_chip = me < 2

    def columns_of(head):
        return pl.ds(pl.multiple_of(head * HD, HD), HD)

    def remote(src, dst, sender, recv, target):
        return pltpu.make_async_remote_copy(
            src_ref=src, dst_ref=dst, send_sem=sender, recv_sem=recv,
            device_id=target, device_id_type=pl.DeviceIdType.MESH,
        )

    def landed(ref, sem):
        remote(ref, ref, send.at[0], sem, {"tm": block}).wait_recv()

    def sent(ref, sem):
        remote(ref, ref, sem, out_sem, {"tm": block}).wait_send()

    if tiles == 2:
        sides = [(tile >= 1, 1 - 2 * tile, None)]
    elif tiles > 2:
        sides = [(None, -1, tile >= 1), (None, 1, tile + 1 < tiles)]
    else:
        sides = []

    def maybe(condition, action):
        if condition is None:
            action()
        else:
            pl.when(condition)(action)

    barrier = pltpu.get_barrier_semaphore()
    expected = jnp.int32(GROUP - 1)

    def greet(target):
        pl.semaphore_signal(barrier, inc=1, device_id=target, device_id_type=pl.DeviceIdType.MESH)

    for role in (across, beyond, partner):
        greet({"tm": base + role})
    for _, step, there in sides:
        maybe(there, lambda: greet({"tile": tile + step}))
        expected += 1 if there is None else there.astype(jnp.int32)
    for there, step in ((behind, -GROUP), (ahead, GROUP)):
        pl.when(there)(lambda: greet({"tm": block + step}))
        expected += there.astype(jnp.int32)

    pltpu.make_async_copy(lists_hbm, lists_ref, small_sem.at[0]).start()
    pltpu.make_async_copy(halo_hbm, halo_ref, small_sem.at[1]).start()

    def spots(h):
        return ((k_ref, kv.at[me, h, 0]), (v_ref, kv.at[me, h, 1]), (q_ref, qs.at[me, h]))

    for at, role in enumerate((across, beyond)):
        for i, ref in enumerate((k_ref, v_ref)):
            pltpu.make_async_copy(ref.at[:, columns_of(role * share)], stage.at[at, i], stage_sem).start()

    def fetch(h, carry):
        for ref, spot in spots(h):
            pltpu.make_async_copy(ref.at[:, columns_of(me * share + h)], spot, local_sem).start()
        return carry

    lax.fori_loop(0, share, fetch, 0)

    pltpu.make_async_copy(lists_hbm, lists_ref, small_sem.at[0]).wait()
    pltpu.make_async_copy(halo_hbm, halo_ref, small_sem.at[1]).wait()
    row = lax.broadcasted_iota(jnp.int32, (ROWS, tokens), 0)
    mine = jnp.where(row == slots, halo_ref[0, 0, 0], -1)
    for n in range(slots):
        mine = jnp.where(row == n, lists_ref[0, 0, n], mine)
    info[me] = mine

    pl.semaphore_wait(barrier, expected)

    def give(role, h, pairs, sem):
        for ref, spot in pairs:
            kind = Q_SENT if ref is q_ref else KV_SENT
            remote(ref.at[:, columns_of(role * share + h)], spot, send.at[kind], sem,
                   {"tm": base + role}).start()

    def give_keys(h):
        for role in (across, beyond):
            give(role, h, spots(h)[:2], kv_sem.at[h])

    def give_queries(h):
        for role in (across, beyond):
            give(role, h, spots(h)[2:], q_sem.at[h])

    def to_sides(role, kind, h):
        for at, (_, step, there) in enumerate(sides):
            other = len(sides) - 1 - at
            maybe(there, lambda: remote(
                kv.at[role, h], side.at[other, role, h], side_send.at[at],
                side_sem.at[other, kind, h], {"tile": tile + step}).start())

    def to_next(role, h):
        @pl.when(both(role == last, ahead))
        def _():
            remote(kv.at[role, h], past.at[h], send.at[PAST_SENT], past_sem.at[h],
                   {"tm": block + GROUP}).start()

    def to_before(role, h):
        @pl.when(behind)
        def _():
            remote(qs.at[role, h], ask.at[role, h], send.at[ASK_SENT], ask_sem.at[h],
                   {"tm": block - GROUP}).start()

    def near_z(h):
        for role in (me, partner):
            to_before(role, h)
            to_next(role, h)

    for role in (across, beyond, partner):
        remote(info.at[me], info.at[me], send.at[INFO_SENT], info_sem.at[0],
               {"tm": base + role}).start()
    pltpu.make_async_copy(stage, stage, stage_sem).wait()
    for at, role in enumerate((across, beyond)):
        remote(stage.at[at], kv.at[me, 0], send.at[KV_SENT], kv_sem.at[0], {"tm": base + role}).start()
    pltpu.make_async_copy(kv.at[me], kv.at[me], local_sem).wait()
    pltpu.make_async_copy(qs.at[me], qs.at[me], local_sem).wait()
    to_sides(me, MINE, 0)
    for h in range(min(3, share)):
        give_queries(h)
    give(partner, 0, spots(0), near_sem.at[0])

    def give_rest(h, carry):
        give(partner, h, spots(h), near_sem.at[1])
        return carry

    def give_far(h, carry):
        give_keys(h)
        pl.when(h + 2 < share)(lambda: give_queries(h + 2))
        return carry

    lax.fori_loop(1, share, give_rest, 0)
    lax.fori_loop(1, share, give_far, 0)
    landed(res.at[pl.ds(0, 3), 0], near_sem.at[0])
    to_sides(partner, NEAR, 0)
    near_z(0)

    landed(info.at[pl.ds(0, GROUP - 1)], info_sem.at[0])

    @pl.when(behind)
    def _():
        remote(info.at[pl.ds(0, GROUP)], info.at[pl.ds(GROUP, GROUP)], send.at[ASKED_SENT],
               info_sem.at[1], {"tm": block - GROUP}).start()

    landed(res.at[pl.ds(0, 3), pl.ds(0, share - 1)], near_sem.at[1])

    def near_sides(h):
        to_sides(partner, NEAR, h)
        to_sides(me, MINE, h)

    near_sides(1)

    @pl.when(jnp.logical_not(behind))
    def _():
        past[...] = jnp.zeros(past.shape, past.dtype)
        back[...] = jnp.zeros(back.shape, back.dtype)
        back_stat[...] = jnp.full(back_stat.shape, LOW, back_stat.dtype)

    for at, (_, _, there) in enumerate(sides):
        if there is not None:

            @pl.when(jnp.logical_not(there))
            def _():
                side[at] = jnp.zeros(side.shape[1:], side.dtype)

    def spread(at, number):
        out = jnp.full((ROWS, tokens), LOW, jnp.float32)
        for d in range(1, WIN + 1):
            wanted = jnp.where(number >= d, number - d, -2)
            hit = info[at, 0:1, :] == wanted
            for n in range(1, slots):
                hit = jnp.logical_or(hit, info[at, n : n + 1, :] == wanted)
            out = jnp.where(jnp.logical_and(row == d, hit), 0.0, out)
        far[at] = out

    query = lax.broadcasted_iota(jnp.int32, (tokens, tokens), 0) // (rows * columns)
    key = lax.broadcasted_iota(jnp.int32, (tokens, tokens), 1)
    causal = key // (rows * columns) <= query
    bias[0] = jnp.where(causal, 0.0, LOW)
    key_row = (lax.broadcasted_iota(jnp.int32, (1, tokens), 1) // columns) % rows
    for role in range(GROUP):
        spread(role, base + role)
        reach = info[role, slots : slots + 1, :]
        above = jnp.where(key_row >= rows - reach, 0.0, LOW)
        below = jnp.where(key_row < reach, 0.0, LOW)
        for at, (upper, step, there) in enumerate(sides):
            if upper is not None:
                edge = jnp.where(upper, above, below)
            else:
                edge = jnp.where(there, above if step < 0 else below, LOW)
            bias[1 + role * len(sides) + at] = jnp.where(causal, edge, LOW)

    @pl.when(ahead)
    def _():
        landed(info.at[pl.ds(GROUP, GROUP)], info_sem.at[1])

        for role in range(GROUP):
            spread(GROUP + role, base + GROUP + role)

    def attend(query_part, parts):
        scores = []
        most = None
        for pair, shift in parts:
            s = lax.dot_general(query_part, pair[0], (((1,), (1,)), ((), ())),
                                preferred_element_type=jnp.float32) + shift
            most = s if most is None else jnp.maximum(most, s)
            scores.append(s)
        top = jnp.max(most, axis=1, keepdims=True) * SCALE
        total = None
        numerator = None
        for s, (pair, _) in zip(scores, parts):
            w = jnp.exp2(s * SCALE - top)
            total = w if total is None else total + w
            term = jnp.dot(w.astype(jnp.bfloat16), pair[1], preferred_element_type=jnp.float32)
            numerator = term if numerator is None else numerator + term
        return numerator, jnp.sum(total, axis=1, keepdims=True), top

    def distant(at, d):
        return far[at, d : d + 1, :]

    def visit(role, h):
        parts = []
        for other in range(GROUP):
            d = role + GROUP - other
            if d <= WIN:
                parts.append((kv.at[other, h], distant(GROUP + role, d)))
        if role + 1 + GROUP <= WIN:
            pl.when(behind)(lambda: landed(past.at[h], past_sem.at[h]))
            parts.append((past.at[h], distant(GROUP + role, role + 1 + GROUP)))
        numerator, total, top = attend(ask[role, h], parts)
        part[role, h] = (numerator / total).astype(part.dtype)
        level = jnp.broadcast_to(top + jnp.log2(total), (tokens, HD))
        stat[role, h] = jnp.transpose(level)[0:1, :]
        kind = role // 2
        remote(part.at[role, h], back.at[role, h], send.at[BACK_SENT + kind], back_sem.at[kind, h],
               {"tm": block + GROUP}).start()
        remote(stat.at[role, h], back_stat.at[role, h], send.at[STAT_SENT + kind],
               stat_sem.at[kind, h], {"tm": block + GROUP}).start()

    two = pl.ds(0, 2)

    def returned(kind, h):
        landed(back.at[two, h], back_sem.at[kind, h])
        landed(back_stat.at[two, h], stat_sem.at[kind, h])

    def sides_here(kind, h):
        roles = {FAR: two, NEAR: partner, MINE: me}[kind]
        for at, (_, _, there) in enumerate(sides):
            maybe(there, lambda: landed(side.at[at, roles, h], side_sem.at[at, kind, h]))

    def merge(one, other):
        peak = jnp.maximum(one[2], other[2])
        ours, theirs = jnp.exp2(one[2] - peak), jnp.exp2(other[2] - peak)
        return one[0] * ours + other[0] * theirs, one[1] * ours + other[1] * theirs, peak

    def unit(role, h, between=None):
        parts = [(kv.at[role, h], bias[0])]
        for other in range(role):
            parts.append((kv.at[other, h], distant(role, role - other)))
        margins = [(side.at[at, role, h], bias[1 + role * len(sides) + at]) for at in range(len(sides))]
        level = jnp.transpose(jnp.broadcast_to(back_stat[role, h], (HD, tokens)))
        so_far = (back[role, h].astype(jnp.float32), 1.0, level)
        if between is None:
            parts += margins
        so_far = merge(so_far, attend(qs[role, h], parts))
        if between is not None:
            between()
            if margins:
                so_far = merge(so_far, attend(qs[role, h], margins))
        numerator, total, _ = so_far
        res[role, h] = (numerator / total).astype(res.dtype)
        place = columns_of(me * share + h)

        @pl.when(me == role)
        def _():
            out_ref[:, place] = res[role, h]

        @pl.when(me != role)
        def _():
            remote(res.at[role, h], out_ref.at[:, place], send.at[RES_SENT], out_sem,
                   {"tm": base + role}).start()

    def rest(t):
        h = t - 1

        def one(n, carry):
            k = jnp.where(n == 2, -1, n - (n > 2).astype(jnp.int32))
            turn = jnp.where(k == 0, across, jnp.where(k == 1, beyond, jnp.where(k == 2, partner, me)))
            final = both(k == 3, t == share)

            @pl.when(t >= 1)
            def _():
                pl.when(both(k == 0, behind))(lambda: returned(1 - me // 2, h))
                pl.when(both(k == 2, behind))(lambda: returned(me // 2, h))
                pl.when(k == 0)(lambda: sides_here(FAR, h))
                pl.when(k == 2)(lambda: sides_here(NEAR, h))
                pl.when(both(k == 3, t < share))(lambda: sides_here(MINE, h))

            pl.when(both(k == 3, t + 2 == share))(lambda: keys_here(t + 1))
            for role in range(GROUP):
                pl.when(both(k >= 0, t >= 1, turn == role, jnp.logical_not(final)))(
                    lambda: unit(role, h))
                pl.when(both(final, turn == role))(
                    lambda: unit(role, h, lambda: sides_here(MINE, h)))

            pl.when(both(k < 0, t < share, ahead, first_chip))(lambda: visit(0, t))
            pl.when(both(k < 0, t < share, ahead, jnp.logical_not(first_chip)))(lambda: visit(last, t))
            return carry

        lax.fori_loop(0, GROUP + 1, one, 0)

    def keys_here(h):
        landed(kv.at[two, h], kv_sem.at[h])
        for role in (across, beyond):
            to_sides(role, FAR, h)
            to_next(role, h)

    def query_here(h):
        landed(qs.at[two, h], q_sem.at[h])
        for role in (across, beyond):
            to_before(role, h)

    def step(t, carry):
        @pl.when(t < share)
        def _():
            pl.when(t + 1 < share)(lambda: keys_here(t))
            pl.when(t + 3 < share)(lambda: to_sides(partner, NEAR, t + 2))
            pl.when(both(t == 0, t + 3 < share))(lambda: to_sides(me, MINE, t + 2))
            pl.when(both(t >= 2, t + 2 < share))(lambda: to_sides(me, MINE, t + 1))
            pl.when(both(t + 1 == share, share > 2))(lambda: near_sides(t))
            pl.when(t == 0)(lambda: query_here(t))

            @pl.when(t + 1 < share)
            def _():
                query_here(t + 1)
                pl.when(t == 0)(lambda: near_z(t + 1))
                pl.when(t + 2 < share)(lambda: near_z(t + 2))

            @pl.when(ahead)
            def _():
                landed(ask.at[:, t], ask_sem.at[t])

                @pl.when(first_chip)
                def _():
                    for role in (2, 3, 1):
                        visit(role, t)

                @pl.when(jnp.logical_not(first_chip))
                def _():
                    for role in (1, 0, 2):
                        visit(role, t)

            pl.when(both(behind, jnp.logical_not(ahead)))(lambda: landed(past.at[t], past_sem.at[t]))

        rest(t)
        return carry

    lax.fori_loop(0, share + 1, step, 0)

    peers = pl.ds(0, GROUP - 1)
    landed(res.at[peers], out_sem)
    sent(res.at[peers], send.at[RES_SENT])
    sent(info.at[peers], send.at[INFO_SENT])
    sent(qs.at[peers], send.at[Q_SENT])
    sent(kv.at[peers], send.at[KV_SENT])
    for at, (_, _, there) in enumerate(sides):
        maybe(there, lambda: sent(side.at[at], side_send.at[at]))

    @pl.when(ahead)
    def _():
        sent(past, send.at[PAST_SENT])
        for kind in range(2):
            sent(back.at[two], send.at[BACK_SENT + kind])
            sent(back_stat.at[two], send.at[STAT_SENT + kind])

    @pl.when(behind)
    def _():
        sent(ask, send.at[ASK_SENT])
        sent(info.at[pl.ds(0, GROUP)], send.at[ASKED_SENT])


def local(count, tiles, queries, keys, values, neighbours, halo_rows):
    frames, rows, columns, channels = queries.shape
    tokens = frames * rows * columns
    heads = channels // HD
    share = heads // GROUP
    assert rows == HMAX and count % GROUP == 0 and heads % GROUP == 0
    sides = min(2, tiles - 1)
    flat = (tokens, channels)
    piece = (tokens, HD)
    anywhere = pl.BlockSpec(memory_space=pltpu.HBM)
    dma = pltpu.SemaphoreType.DMA

    def vmem(*size, dtype=jnp.bfloat16):
        return pltpu.VMEM(size, dtype)

    out = pl.pallas_call(
        functools.partial(kernel, count, tiles, (frames, rows, columns)),
        out_shape=pltpu.VMEM(flat, jnp.bfloat16),
        in_specs=[anywhere] * 5,
        out_specs=pl.BlockSpec(memory_space=pltpu.VMEM),
        scratch_shapes=[
            pltpu.SMEM(neighbours.shape, jnp.int32),
            pltpu.SMEM((1, 1, 1), jnp.int32),
            vmem(GROUP, share, *piece),
            vmem(GROUP, share, 2, *piece),
            vmem(max(1, sides), GROUP, share, 2, *piece),
            vmem(share, 2, *piece),
            vmem(GROUP, share, *piece),
            vmem(GROUP, share, *piece),
            vmem(GROUP, share, 1, tokens, dtype=jnp.float32),
            vmem(GROUP, share, *piece),
            vmem(GROUP, share, 1, tokens, dtype=jnp.float32),
            vmem(GROUP, share, *piece),
            vmem(2 * GROUP, ROWS, tokens, dtype=jnp.int32),
            vmem(2 * GROUP, ROWS, tokens, dtype=jnp.float32),
            vmem(1 + GROUP * sides, tokens, tokens, dtype=jnp.float32),
            vmem(2, 2, *piece),
            dma,
            dma((2,)),
            dma((KINDS,)),
            dma((max(1, sides),)),
            dma,
            dma((2,)),
            dma((share,)),
            dma((share,)),
            dma((max(1, sides), 3, share)),
            dma((share,)),
            dma((share,)),
            dma((2, share)),
            dma((2, share)),
            dma,
            dma((2,)),
        ],
        compiler_params=pltpu.CompilerParams(
            collective_id=0, has_side_effects=True, vmem_limit_bytes=56 * 1024 * 1024
        ),
    )(
        neighbours,
        halo_rows.reshape(1, 1, 1),
        queries.reshape(flat),
        keys.reshape(flat),
        values.reshape(flat),
    )
    return out.reshape(queries.shape)


def solution(mesh):
    return jax.shard_map(
        functools.partial(local, mesh.shape["tm"], mesh.shape["tile"]),
        mesh=mesh,
        in_specs=(
            P("tm", "tile", None, None),
            P("tm", "tile", None, None),
            P("tm", "tile", None, None),
            P("tm", "tile", None),
            P("tm", "tile"),
        ),
        out_specs=P("tm", "tile", None, None),
        check_vma=False,
    )
```
